256 devices in a mesh: pool: 16 (over y, x), slab: 16 (over z, core).
Axes of the slice: x: 4, y: 4, z: 8, core: 2. Of those that a mesh axis runs over, the one named last changes fastest.
Arguments:
- wave_coeff: bfloat16 [256, 2, 96, 9216], P(('pool', 'slab')), may hold values from -6 to 6
- response_coeff: bfloat16 [256, 2, 96, 9216], P(('pool', 'slab')), may hold values from -6 to 6
- band_index: int32 [256], P(('pool', 'slab')), may hold values from 0 to 255, each once
- occupation: int32 [256], replicated, may hold values from 0 to 2
- local_kernel: float32 [96, 9216], P('slab'), may hold values from 0.5 to 4
- gradient_kernel: float32 [96, 9216], P('slab'), may hold values from 0.25 to 2.5
Outputs:
- induced_potential: float32 [96, 9216], P('slab', 'pool')
The draws below stay inside these ranges and needn't reach their ends.
Inputs may be any that keep to these rules, and one draw needn't show every extreme that they name: `band_index`: a permutation of the 256 band numbers.
All inputs are finite; a program needn't handle non-finite values.
Results may differ from the reference program's by a relative error of at most 0.0067.
Values sent between devices are 32-bit elements; how exact they have to be, the bound alone decides.
A program may use at most 128 MiB of HBM per device.

```python
import math
import jax
import jax.numpy as jnp
from jax import lax

NG = 96
BANDS = 256


def with_ends(entries, key, low, largest):
    longest = entries.shape.index(max(entries.shape))
    spots = []
    for shift in (0, 1):
        where = [jax.random.randint(jax.random.fold_in(key, axis), (), 0, length) for axis, length in enumerate(entries.shape)]
        where[longest] = (where[longest] + shift) % entries.shape[longest]
        spots.append(tuple(where))
    return entries.at[spots[0]].set(low).at[spots[1]].set(largest)


def shard_levels(key, dims, cuts, low, largest):
    factor_of = 1.0
    for axis_at, parts in cuts:
        heights = jax.random.uniform(jax.random.fold_in(jax.random.fold_in(key, 6), axis_at), (parts,), jnp.float32, low / len(cuts), largest / len(cuts))
        factor_of = factor_of * jnp.repeat(jnp.exp(heights), dims[axis_at] // parts).reshape((-1,) + (1,) * (len(dims) - 1 - axis_at))
    return factor_of


def gaussian(key, dims, deviation, reach, cuts=(), kind=jnp.bfloat16):
    drawn = jax.random.normal(key, dims, jnp.float32) * deviation
    if len(cuts) > 0:
        drawn = shard_levels(key, dims, cuts, -0.22, 0.18) * drawn
    return jnp.clip(drawn, min=-reach, max=reach).astype(kind)


def setup_inputs(seed: int = 0) -> dict:
    streams_of = jax.random.split(jax.random.key(seed), 7)
    wave_coeff = gaussian(streams_of[0], (BANDS, 2, NG, NG * NG), 1.0, 6.0, ((0, 256),))
    response_coeff = gaussian(streams_of[1], (BANDS, 2, NG, NG * NG), 1.0, 6.0, ((0, 256),))
    band_index = jax.random.permutation(streams_of[2], BANDS).astype(jnp.int32)
    occupation = with_ends(jax.random.randint(streams_of[3], (BANDS,), 0, 3), jax.random.fold_in(streams_of[3], 1), 0, 2).astype(jnp.int32)
    local_kernel = jnp.clip(jnp.exp(math.log(4.0) - 2.0794415 * jax.random.uniform(streams_of[4], (NG, NG * NG), jnp.float32) ** shard_levels(streams_of[4], (NG, NG * NG), ((0, 16),), -0.2, 0.2)), 0.5, 4.0)
    gradient_kernel = jnp.clip(jnp.exp(math.log(2.5) - 2.3025851 * jax.random.uniform(streams_of[5], (NG, NG * NG), jnp.float32) ** shard_levels(streams_of[5], (NG, NG * NG), ((0, 16),), -0.2, 0.2)), 0.25, 2.5)
    return {"wave_coeff": wave_coeff, "response_coeff": response_coeff, "band_index": band_index, "occupation": occupation, "local_kernel": local_kernel, "gradient_kernel": gradient_kernel}


full_turn = 2.0 * math.pi

def stacked_table(length, sign, dtype):
    indices = jnp.arange(length, dtype=jnp.int32)
    product = indices[:, None] * indices[None, :] % length
    angles = product.astype(jnp.float32) * (full_turn / length)
    factor = 1.0 / math.sqrt(length)
    cosine = jnp.cos(angles) * factor
    sine_part = jnp.sin(angles) * factor
    upper_half = jnp.stack([cosine, -sign * sine_part], axis=1)
    lower_half = jnp.stack([sign * sine_part, cosine], axis=1)
    return jnp.stack([upper_half, lower_half], axis=0).astype(dtype)

def signed_freq(length, first_wave, amount):
    waves = first_wave + jnp.arange(amount, dtype=jnp.int32)
    return jnp.where(2 * waves >= length, waves - length, waves).astype(jnp.float32)

def coulomb_kernel(length, starts, counts):
    first_freq = signed_freq(length, starts[0], counts[0])[:, None, None]
    second_freq = signed_freq(length, starts[1], counts[1])[None, :, None]
    third_freq = signed_freq(length, starts[2], counts[2])[None, None, :]
    squared = (full_turn / length) ** 2 * (first_freq * first_freq + second_freq * second_freq + third_freq * third_freq)
    nonzero = jnp.where(squared > 0, squared, 1.0)
    return jnp.where(squared > 0, full_turn / nonzero, 0.0)

def to_space(tables, coeffs):
    first_pass = jnp.einsum('rzsk,skxy->rzxy', tables, coeffs.astype(jnp.float32)).astype(jnp.bfloat16)
    first_pass = lax.optimization_barrier(first_pass)
    second_pass = jnp.einsum('rxsk,szky->rzxy', tables, first_pass.astype(jnp.float32)).astype(jnp.bfloat16)
    second_pass = lax.optimization_barrier(second_pass)
    return jnp.einsum('rysk,szxk->rzxy', tables, second_pass.astype(jnp.float32))

def central(values, which_axis):
    return (jnp.roll(values, -1, which_axis) - jnp.roll(values, 1, which_axis)) * 0.5

def reference(wave_coeff, response_coeff, band_index, occupation, local_kernel, gradient_kernel):
    length = wave_coeff.shape[2]
    band_total = wave_coeff.shape[0]
    tables = stacked_table(length, 1.0, jnp.bfloat16).astype(jnp.float32)
    weights = occupation[band_index].astype(jnp.float32)
    cube_shape = (2, length, length, length)

    def one_band(running, band_items):
        wave_part, response_part, weight = band_items
        wave_space = to_space(tables, wave_part.reshape(cube_shape))
        response_space = to_space(tables, response_part.reshape(cube_shape))
        intersection = wave_space[0] * response_space[0] + wave_space[1] * response_space[1]
        return (running + weight * intersection, None)
    running = lax.scan(one_band, jnp.zeros((length, length, length), jnp.float32), (wave_coeff, response_coeff, weights))[0]
    density = running / band_total
    spectrum = jnp.fft.fftn(density, norm='ortho')
    kernel = coulomb_kernel(length, (0, 0, 0), (length, length, length))
    hartree = jnp.real(jnp.fft.ifftn(spectrum * kernel, norm='ortho'))
    coefficient = gradient_kernel.reshape(length, length, length)
    divergence = central(coefficient * central(density, 0), 0)
    divergence = divergence + central(coefficient * central(density, 1), 1)
    divergence = divergence + central(coefficient * central(density, 2), 2)
    potential = hartree + local_kernel.reshape(length, length, length) * density - divergence
    return potential.reshape(length, length * length)
```

```python
import math
import numpy as np
import jax, jax.numpy as jnp
from jax import lax
from jax.experimental import pallas as pl
from jax.experimental.pallas import tpu as pltpu
from jax.sharding import PartitionSpec as P

MESH = pl.DeviceIdType.MESH
full_turn = 2.0 * math.pi
N = 96

def np_tables():
    k = np.arange(N)
    ang = (np.outer(k, k) % N) * (2 * np.pi / N)
    c, s = np.cos(ang) / np.sqrt(N), np.sin(ang) / np.sqrt(N)
    t = np.block([[c, -s], [s, c]]).astype(np.float32)
    hu = (np.cos(ang) + np.sin(ang)).astype(np.float32)
    return t, hu

def y_tables(t):
    outs = []
    for row in range(4):
        js = sorted({(96 * row) // 128, (96 * row + 95) // 128})
        w = np.zeros((256 * len(js), 256), np.float32)
        for n, j in enumerate(js):
            for l in range(128):
                d = 128 * j + l
                if d // 96 != row:
                    continue
                ky = d % 96
                for s in range(2):
                    for r in range(2):
                        w[256 * n + 128 * s + l, 128 * r:128 * r + 96] = t[96 * r:96 * r + 96, 96 * s + ky]
        outs.append(w)
    return outs

def dense_tables(hu):
    outs = []
    for j in range(3):
        w = np.zeros((256, 128), np.float32)
        for l in range(128):
            d = 128 * j + l
            q, ky = d // 96, d % 96
            w[(q - j) * 128:(q - j) * 128 + 96, l] = hu[ky]
        outs.append(w)
    return np.stack(outs)

BL = 1536
NB = 9216 // BL

def kernel_a(occ, idx, wave, resp, t_ref, w0, w1, w2, w3, yd, hx, out, bw, br):
    step = pl.program_id(0)
    f32, bf = jnp.float32, jnp.bfloat16

    @pl.when(step < NB)
    def _():
        t = t_ref[...]
        for src, dst in ((wave, bw), (resp, br)):
            c = jnp.concatenate([src[0, 0], src[0, 1]], axis=0)
            zb = jnp.dot(t, c, preferred_element_type=f32).astype(bf)
            groups = BL // 384
            for row, w in enumerate((w0, w1, w2, w3)):
                js = sorted({(96 * row) // 128, (96 * row + 95) // 128})
                lhs = jnp.concatenate([
                    jnp.concatenate([zb[96 * s:96 * s + 96, 384 * g + 128 * j:384 * g + 128 * j + 128] for j in js for s in range(2)], axis=1)
                    for g in range(groups)], axis=0)
                res = jnp.dot(lhs, w[...], preferred_element_type=f32)
                for g in range(groups):
                    base = step * (BL // 96 * 96) + (4 * g + row) * 96
                    for r in range(2):
                        dst[r, pl.ds(pl.multiple_of(base, 96), 96), :] = res[96 * g:96 * g + 96, 128 * r:128 * r + 128]

    @pl.when(step >= NB)
    def _():
        chunk = step - NB
        weight = occ[idx[0]].astype(f32) * (1.0 / 256.0)

        def body(i, carry):
            t = t_ref[...]
            spaces = []
            for src in (bw, br):
                parts = []
                for q in range(4):
                    z = chunk * 32 + 8 * q + i
                    parts.append(jnp.concatenate([src[r, pl.ds(z, 96, stride=96), :].astype(bf) for r in range(2)], axis=0))
                spaces.append(jnp.dot(t, jnp.concatenate(parts, axis=1), preferred_element_type=f32))
            a, b = spaces
            rho = (a[:96] * b[:96] + a[96:] * b[96:]) * weight
            hi = rho.astype(bf)
            lo = (rho - hi.astype(f32)).astype(bf)
            cols = []
            for j in range(3):
                lhs = jnp.concatenate([hi[:, 128 * j:128 * j + 256], lo[:, 128 * j:128 * j + 256]], axis=1)
                cols.append(jnp.dot(lhs, yd[j], preferred_element_type=f32))
            r = jnp.concatenate(cols, axis=1)
            rhi = r.astype(bf)
            rlo = (r - rhi.astype(f32)).astype(bf)
            g = jnp.dot(hx[...], jnp.concatenate([rhi, rlo], axis=0), preferred_element_type=f32)
            for j in range(3):
                out[j, pl.ds(i, 96, stride=8), :] = g[:, 128 * j:128 * j + 128]
            return carry
        lax.fori_loop(0, 8, body, 0)

def run_a(wave, resp, occ, idx):
    t, hu = np_tables()
    bf = jnp.bfloat16
    ws = [jnp.asarray(w, bf) for w in y_tables(t)]
    yd = dense_tables(hu)
    yd = jnp.asarray(np.concatenate([yd, yd], axis=1), bf)
    hx = jnp.asarray(np.concatenate([hu, hu], axis=1), bf)
    tb = jnp.asarray(t, bf)
    full = lambda a: pl.BlockSpec(a.shape, lambda i: (0,) * a.ndim)
    consts = [tb, *ws, yd, hx]
    return pl.pallas_call(
        kernel_a,
        grid=(NB + 3,),
        out_shape=jax.ShapeDtypeStruct((9, 768, 128), jnp.float32),
        in_specs=[pl.BlockSpec(memory_space=pltpu.SMEM), pl.BlockSpec(memory_space=pltpu.SMEM),
                  pl.BlockSpec((1, 2, 96, BL), lambda i: (0, 0, 0, jnp.minimum(i, NB - 1))),
                  pl.BlockSpec((1, 2, 96, BL), lambda i: (0, 0, 0, jnp.minimum(i, NB - 1))),
                  *[full(a) for a in consts]],
        out_specs=pl.BlockSpec((3, 768, 128), lambda i: (jnp.maximum(i - NB, 0), 0, 0)),
        scratch_shapes=[pltpu.VMEM((2, 9216, 128), jnp.float32), pltpu.VMEM((2, 9216, 128), jnp.float32)],
        compiler_params=pltpu.CompilerParams(vmem_limit_bytes=60 * 1024 * 1024),
        name="bands",
    )(occ, idx, wave, resp, *consts)

def window_tables(hu):
    h = hu / np.sqrt(N).astype(np.float64)
    rows = np.array([(12 * zc - 2 + w) % N for zc in range(8) for w in range(16)])
    sel = np.zeros((128, N), np.float32)
    sel[np.arange(128), rows] = 1.0
    hye = np.zeros((128, 128), np.float64)
    cols = (np.arange(128) - 16) % N
    hye[:N] = hu[:, cols] / N
    return h.astype(np.float32), h[rows].astype(np.float32), sel, hye.astype(np.float32)


def exact(a, b):
    return jnp.dot(a, b, precision=lax.Precision.HIGHEST, preferred_element_type=jnp.float32)


def kernel_b(d, g, l, hz, hze, sel, hye, hx, out, pbuf, s, f1, t, f2, zbuf, zs, zr, q, a, gr,
             p_snd, p_rcv, s1, r1, s2, r2, sz, rz, sa, ra, sg, rg):
    pool, slab = lax.axis_index("pool"), lax.axis_index("slab")
    y, x = pool // 4, pool % 4
    zc, core = slab // 2, slab % 2
    other = 1 - core
    partner = zc * 2 + other

    def dev(p, sl):
        return {"pool": p, "slab": sl}

    def plane(k):
        dc, dp = k // 16, k % 16
        c2 = (core + dc) % 2
        return c2, dev((pool + dp) % 16, zc * 2 + c2)

    barrier = pltpu.get_barrier_semaphore()
    def hail(who):
        pl.semaphore_signal(barrier, inc=1, device_id=who, device_id_type=MESH)
    for k in range(1, 32):
        hail(plane(k)[1])
    for dz in range(1, 8):
        hail(dev(pool, (slab + 2 * dz) % 16))
    hail(dev(pool, (slab + 15 + 2 * core) % 16))
    pl.semaphore_wait(barrier, 39)

    def send(src, dst, ssem, rsem, who):
        cp = pltpu.make_async_remote_copy(src_ref=src, dst_ref=dst, send_sem=ssem, recv_sem=rsem, device_id=who, device_id_type=MESH)
        cp.start()
        return cp

    pair = [send(d.at[u, other], pbuf.at[u], p_snd.at[u], p_rcv.at[u], dev(pool, partner)) for u in range(9)]
    gs = [send(g, gr.at[0], sg.at[0], rg.at[0], dev(pool, (slab + 1) % 16)),
          send(g, gr.at[1], sg.at[1], rg.at[1], dev(pool, (slab + 15) % 16))]

    first = []
    for u in range(9):
        pair[u].wait_recv()
        s[u] = d[u, core] + pbuf[u]
        cps = []
        for k in range(1, 4):
            if u % 2 == 0:
                o = (x + k) % 4
                cps.append(send(s.at[u, :, o], f1.at[u, k - 1], s1.at[u, k - 1], r1.at[u, k - 1], dev(y * 4 + o, slab)))
            else:
                o = (y + k) % 4
                cps.append(send(s.at[u, o], f1.at[u, k - 1], s1.at[u, k - 1], r1.at[u, k - 1], dev(o * 4 + x, slab)))
        first.append(cps)

    second = []
    for u in range(9):
        for cp in first[u]:
            cp.wait_recv()
        own = s[u, :, x] if u % 2 == 0 else s[u, y]
        t[u] = own + f1[u, 0] + f1[u, 1] + f1[u, 2]
        cps = []
        for k in range(1, 4):
            if u % 2 == 0:
                o = (y + k) % 4
                who = dev(o * 4 + x, slab)
            else:
                o = (x + k) % 4
                who = dev(y * 4 + o, slab)
            cps.append(send(t.at[u, o], f2.at[u, k - 1], s2.at[u, k - 1], r2.at[u, k - 1], who))
        second.append(cps)

    lane = lax.broadcasted_iota(jnp.int32, (8, 128), 1)
    for c in range(3):
        parts = []
        for j in range(3):
            u = 3 * c + j
            for cp in second[u]:
                cp.wait_recv()
            own = t[u, y] if u % 2 == 0 else t[u, x]
            parts.append(own + f2[u, 0] + f2[u, 1] + f2[u, 2])
        for m in range(3):
            v = jnp.concatenate([parts[j][m] for j in range(3)], axis=1)
            for k in range(4):
                w = v if k == 0 else pltpu.roll(v, 384 - 96 * k, 1)
                zbuf[32 * c + 8 * k:32 * c + 8 * k + 8, 128 * m:128 * m + 128] = jnp.where(lane < 96, w[:, :128], 0.0)

    zk = zbuf[...]
    vh = exact(hz[...], zk)
    kz = lax.broadcasted_iota(jnp.int32, (96, 128), 0)
    ky = lax.broadcasted_iota(jnp.int32, (96, 128), 1)
    qz = jnp.where(2 * kz >= N, kz - N, kz)
    qy = jnp.where(2 * ky >= N, ky - N, ky)
    zy = qz * qz + qy * qy
    scaled = []
    for m in range(3):
        kx = jnp.full((96, 128), 1, jnp.int32) * (3 * (core * 16 + pool) + m)
        qx = jnp.where(2 * kx >= N, kx - N, kx)
        squared = (zy + qx * qx).astype(jnp.float32) * ((full_turn / N) ** 2)
        kernel = jnp.where(squared > 0, full_turn / jnp.where(squared > 0, squared, 1.0), 0.0)
        scaled.append(vh[:, 128 * m:128 * m + 128] * kernel)
    vz = exact(hze[...], jnp.concatenate(scaled, axis=1))
    dz_ = exact(sel[...], zk)
    rows = jnp.concatenate([dz_[:, :128], dz_[:, 128:256], dz_[:, 256:], vz[:, :128], vz[:, 128:256], vz[:, 256:]], axis=0)
    both = exact(rows, hye[...])
    for b in range(6):
        for zd in range(8):
            zs[zd, b] = both[128 * b + 16 * zd:128 * b + 16 * zd + 16]

    zcp = []
    for k in range(1, 8):
        o = (zc + k) % 8
        zcp.append(send(zs.at[o], zr.at[k - 1], sz.at[k - 1], rz.at[k - 1], dev(pool, o * 2 + core)))
    f = zs[zc]
    for k in range(7):
        zcp[k].wait_recv()
        f = f + zr[k]
    for c2 in range(2):
        for m in range(3):
            q[c2, m] = jnp.concatenate([f[m][6 * c2:6 * c2 + 10], f[3 + m][6 * c2 + 2:6 * c2 + 8]], axis=0)
    me = 3 * (core * 16 + pool)
    acp = []
    for k in range(1, 32):
        c2, who = plane(k)
        acp.append(send(q.at[c2], a.at[pl.ds(me, 3)], sa.at[k - 1], ra.at[k - 1], who))
    a[pl.ds(me, 3)] = q[core]
    for cp in acp:
        cp.wait_recv()
    for cp in gs:
        cp.wait_recv()

    def turn(kx, acc):
        blk = a[kx]
        return tuple(acc[i] + hx[((6 * pool + 94 + i) % 96) * 96 + kx] * blk for i in range(10))
    acc = lax.fori_loop(0, 96, turn, tuple(jnp.zeros((16, 128), jnp.float32) for _ in range(10)))

    across = []
    for i in range(8):
        across.append(g[i][0:6] * ((acc[i + 2][2:8] - acc[i][2:8]) * 0.5))
    for i in range(6):
        rho = acc[i + 2]
        coef = g[i + 1]
        gz = jnp.concatenate([gr[0, i + 1][5:6], coef[0:6], gr[1, i + 1][0:1]], axis=0)
        flux = gz * ((rho[2:10] - rho[0:8]) * 0.5)
        div = (flux[2:8] - flux[0:6]) * 0.5
        div = div + (across[i + 2] - across[i]) * 0.5
        slope = (pltpu.roll(rho, 127, 1) - pltpu.roll(rho, 1, 1)) * 0.5
        along = coef * slope[2:10]
        div = div + ((pltpu.roll(along, 127, 1) - pltpu.roll(along, 1, 1)) * 0.5)[0:6]
        out[i, 0:6, :] = rho[10:16] + l[i][0:6] * rho[2:8] - div
        out[i, 6:8, :] = jnp.zeros((2, 128), jnp.float32)

    for cps in [pair, gs, *first, *second, zcp, acp]:
        for cp in cps:
            cp.wait_send()


def run_b(d, g, l):
    _, hu = np_tables()
    tabs = [jnp.asarray(a) for a in window_tables(hu)]
    hx = jnp.asarray((hu / N).astype(np.float32).reshape(-1))
    f32 = jnp.float32
    vm = pl.BlockSpec(memory_space=pltpu.VMEM)
    dma = pltpu.SemaphoreType.DMA
    return pl.pallas_call(
        kernel_b,
        out_shape=jax.ShapeDtypeStruct((6, 8, 128), f32),
        in_specs=[vm] * 7 + [pl.BlockSpec(memory_space=pltpu.SMEM)],
        out_specs=vm,
        scratch_shapes=[
            pltpu.VMEM((9, 4, 4, 3, 8, 128), f32), pltpu.VMEM((9, 4, 4, 3, 8, 128), f32),
            pltpu.VMEM((9, 3, 4, 3, 8, 128), f32), pltpu.VMEM((9, 4, 3, 8, 128), f32),
            pltpu.VMEM((9, 3, 3, 8, 128), f32), pltpu.VMEM((96, 384), f32),
            pltpu.VMEM((8, 6, 16, 128), f32), pltpu.VMEM((7, 6, 16, 128), f32),
            pltpu.VMEM((2, 3, 16, 128), f32), pltpu.VMEM((96, 16, 128), f32), pltpu.VMEM((2, 8, 8, 128), f32),
            dma((9,)), dma((9,)), dma((9, 3)), dma((9, 3)), dma((9, 3)), dma((9, 3)), dma((7,)), dma((7,)),
            dma((31,)), dma((31,)), dma((2,)), dma((2,)),
        ],
        compiler_params=pltpu.CompilerParams(collective_id=0, has_side_effects=True, vmem_limit_bytes=60 * 1024 * 1024),
        name="gather",
    )(d, g, l, *tabs, hx)


def rows_of(kernel3, first, count):
    wide = jnp.concatenate([kernel3[:, 95:], kernel3, kernel3[:, :1]], axis=1)
    part = jnp.transpose(lax.dynamic_slice_in_dim(wide, first + 1, count, 1), (1, 0, 2))
    part = jnp.concatenate([part[..., 80:], part, part[..., :16]], axis=2)
    return jnp.pad(part, ((0, 0), (0, 2), (0, 0)))


def shards(wave_coeff, response_coeff, band_index, occupation, local_kernel, gradient_kernel):
    d = run_a(wave_coeff, response_coeff, occupation, band_index)
    row = 6 * lax.axis_index("pool")
    g = rows_of(gradient_kernel.reshape(6, N, N), row - 1, 8)
    l = rows_of(local_kernel.reshape(6, N, N), row, 6)
    res = run_b(d.reshape(9, 2, 4, 4, 3, 8, 128), g, l)
    return jnp.transpose(res[:, :6, 16:112], (1, 0, 2)).reshape(6, 576)


def solution(mesh):
    return jax.shard_map(
        shards,
        mesh=mesh,
        in_specs=(
            P(("pool", "slab"), None, None, None),
            P(("pool", "slab"), None, None, None),
            P(("pool", "slab")),
            P(),
            P("slab", None),
            P("slab", None),
        ),
        out_specs=P("slab", "pool"),
        check_vma=False,
    )
```

```python
import math

import numpy as np
import jax
import jax.numpy as jnp
from jax import lax
from jax.experimental import pallas as pl
from jax.experimental.pallas import tpu as pltpu
from jax.sharding import PartitionSpec as P

MESH = pl.DeviceIdType.MESH
full_turn = 2.0 * math.pi
N = 96
BL = 1536
NB = 9216 // BL


def np_tables():
    k = np.arange(N)
    ang = (np.outer(k, k) % N) * (2 * np.pi / N)
    c, s = np.cos(ang) / np.sqrt(N), np.sin(ang) / np.sqrt(N)
    t = np.block([[c, -s], [s, c]])
    return t, np.cos(ang) + np.sin(ang)


def y_tables(t):
    outs = []
    for row in range(4):
        js = sorted({(96 * row) // 128, (96 * row + 95) // 128})
        w = np.zeros((256 * len(js), 256))
        for n, j in enumerate(js):
            for l in range(128):
                d = 128 * j + l
                if d // 96 != row:
                    continue
                for s in range(2):
                    for r in range(2):
                        w[256 * n + 128 * s + l, 128 * r:128 * r + 96] = t[96 * r:96 * r + 96, 96 * s + d % 96]
        outs.append(w)
    return outs


def dense_tables(hu):
    outs = []
    for j in range(3):
        w = np.zeros((256, 128))
        for l in range(128):
            q, ky = divmod(128 * j + l, 96)
            w[(q - j) * 128:(q - j) * 128 + 96, l] = hu[ky]
        outs.append(np.concatenate([w, w], axis=0))
    return np.stack(outs)


def window_tables(hu):
    h = hu / math.sqrt(N)
    rows = np.array([(12 * zc - 2 + w) % N for zc in range(8) for w in range(16)])
    sel = np.zeros((128, N))
    sel[np.arange(128), rows] = 1.0
    hye = np.zeros((128, 128))
    hye[:N] = hu[:, (np.arange(128) - 16) % N] / N
    return [h, h[rows], sel, hye]


def x_table(hu):
    w = np.zeros((16, 16, 32, 8))
    for p in range(16):
        for i in range(10):
            w[p, i, :, :3] = (hu[(6 * p - 2 + i) % N] / N).reshape(32, 3)
    w = w.reshape(256, 256)
    hi = w.astype(jnp.bfloat16).astype(np.float64)
    return np.concatenate([hi, hi, w - hi], axis=1)


def exact(a, b):
    return jnp.dot(a, b, precision=lax.Precision.HIGHEST, preferred_element_type=jnp.float32)


def halves(v):
    hi = v.astype(jnp.bfloat16)
    return hi, (v - hi.astype(jnp.float32)).astype(jnp.bfloat16)


def swap(t):
    return t + 1 - 2 * (t % 2)


def mirror(t):
    return 3 - t


def kernel(occ, idx, wave, resp, g, l, t_ref, w0, w1, w2, w3, yd, hx, hz, hze, sel, hye, hxe, out,
           cw, cr, bw, br, d, pbuf, s, f1, t1, f2, t2, f3, u1, f4, zbuf, zs, zrel, zr, q, a, xo, b, gr,
           csem, p_snd, p_rcv, s1, r1, s2, r2, s3, r3, s4, r4, sz, rz, sa, ra, sb, rb, sg, rg):
    f32, bf = jnp.float32, jnp.bfloat16
    pool, slab = lax.axis_index("pool"), lax.axis_index("slab")
    y, x = pool // 4, pool % 4
    zc, core = slab // 2, slab % 2
    other = 1 - core

    def load(k, blk):
        return pltpu.make_async_copy((wave, resp)[k].at[0, :, :, pl.ds(pl.multiple_of(blk * BL, BL), BL)], (cw, cr)[k].at[blk], csem.at[k, blk])

    for blk in range(NB):
        for k in range(2):
            load(k, blk).start()

    def dev(p, sl):
        return {"pool": p, "slab": sl}

    def plane(k):
        dc, dp = k // 16, k % 16
        c2 = (core + dc) % 2
        p2 = (pool + dp) % 16
        return c2, p2, dev(p2, zc * 2 + c2)

    barrier = pltpu.get_barrier_semaphore()

    def hail(who):
        pl.semaphore_signal(barrier, inc=1, device_id=who, device_id_type=MESH)

    for k in range(1, 32):
        hail(plane(k)[2])
    for dz in (1, 2, 3, 5, 6, 7):
        hail(dev(pool, (slab + 2 * dz) % 16))
    hail(dev(pool, (slab + 15 + 2 * core) % 16))

    def send(src, dst, ssem, rsem, who):
        cp = pltpu.make_async_remote_copy(src_ref=src, dst_ref=dst, send_sem=ssem, recv_sem=rsem, device_id=who, device_id_type=MESH)
        cp.start()
        return cp

    q[...] = jnp.zeros_like(q)

    def first_phase(blk, carry):
        for k in range(2):
            load(k, blk).wait()
        t = t_ref[...]
        for src, dst in ((cw, bw), (cr, br)):
            c = jnp.concatenate([src[blk, 0], src[blk, 1]], axis=0)
            zb = jnp.dot(t, c, preferred_element_type=f32).astype(bf)
            groups = BL // 384
            for row, w in enumerate((w0, w1, w2, w3)):
                js = sorted({(96 * row) // 128, (96 * row + 95) // 128})
                lhs = jnp.concatenate([
                    jnp.concatenate([zb[96 * r:96 * r + 96, 384 * n + 128 * j:384 * n + 128 * j + 128] for j in js for r in range(2)], axis=1)
                    for n in range(groups)], axis=0)
                res = jnp.dot(lhs, w[...], preferred_element_type=f32)
                for n in range(groups):
                    base = pl.multiple_of(blk * BL + (4 * n + row) * 96, 96)
                    for r in range(2):
                        dst[r, pl.ds(base, 96), :] = res[96 * n:96 * n + 96, 128 * r:128 * r + 128]
        return carry

    weight = occ[idx[0]].astype(f32) * (1.0 / 256.0)

    def second_phase(chunk, first, last):
        def body(i, carry):
            t = t_ref[...]
            spaces = []
            for src in (bw, br):
                parts = []
                for k in range(4):
                    z = chunk * 32 + 8 * k + i
                    parts.append(jnp.concatenate([src[r, pl.ds(z, 96, stride=96), :].astype(bf) for r in range(2)], axis=0))
                spaces.append(jnp.dot(t, jnp.concatenate(parts, axis=1), preferred_element_type=f32))
            v, w = spaces
            rho = (v[:96] * w[:96] + v[96:] * w[96:]) * weight
            hi, lo = halves(rho)
            cols = []
            for j in range(3):
                lhs = jnp.concatenate([hi[:, 128 * j:128 * j + 256], lo[:, 128 * j:128 * j + 256]], axis=1)
                cols.append(jnp.dot(lhs, yd[j], preferred_element_type=f32))
            gx = jnp.dot(hx[...], jnp.concatenate(halves(jnp.concatenate(cols, axis=1)), axis=0), preferred_element_type=f32)
            for j in range(3):
                d[3 * chunk + j, pl.ds(i, 96, stride=8), :] = gx[:, 128 * j:128 * j + 128]
            return carry
        lax.fori_loop(first, last, body, 0)

    log = {}

    def variant(u):
        return (u % 4) % 2, (u % 4) // 2

    def order(u, along):
        ax, par = variant(u)
        pos = (x, y)[(ax + along) % 2]
        p1, p2 = (swap, mirror) if par == 0 else (mirror, swap)
        return pos, p1, p2, (ax + along) % 2

    def at(ax, pos):
        return dev(y * 4 + pos, slab) if ax == 0 else dev(pos * 4 + x, slab)

    def units(c):
        return range(3 * c, 3 * c + 3)

    def start_pair(c):
        for u in units(c):
            log["p", u] = send(d.at[u, pl.ds(pl.multiple_of(other * 384, 384), 384)], pbuf.at[u], p_snd.at[u], p_rcv.at[u], dev(pool, zc * 2 + other))

    def start_a1(c):
        for u in units(c):
            log["p", u].wait_recv()
            s[u] = (d[u, pl.ds(pl.multiple_of(core * 384, 384), 384), :] + pbuf[u]).reshape(4, 4, 3, 8, 128)
            pos, p1, p2, ax = order(u, 0)
            to = p1(pos)
            for n, blk in enumerate((to, p2(to))):
                src = s.at[u, :, blk] if ax == 0 else s.at[u, blk]
                log["a1", u, n] = send(src, f1.at[u, n], s1.at[u, n], r1.at[u, n], at(ax, to))

    def start_a2(c):
        for u in units(c):
            pos, p1, p2, ax = order(u, 0)
            for n, blk in ((1, p2(pos)), (0, pos)):
                log["a1", u, n].wait_recv()
                own = s[u, :, blk] if ax == 0 else s[u, blk]
                t1[u, n] = own + f1[u, n]
                if n == 1:
                    log["a2", u] = send(t1.at[u, 1], f2.at[u], s2.at[u], r2.at[u], at(ax, p2(pos)))

    def start_b1(c):
        for u in units(c):
            log["a2", u].wait_recv()
            t2[u] = t1[u, 0] + f2[u]
            pos, p1, p2, ax = order(u, 1)
            to = p1(pos)
            for n, blk in enumerate((to, p2(to))):
                log["b1", u, n] = send(t2.at[u, blk], f3.at[u, n], s3.at[u, n], r3.at[u, n], at(ax, to))

    def start_b2(c):
        for u in units(c):
            pos, p1, p2, ax = order(u, 1)
            for n, blk in ((1, p2(pos)), (0, pos)):
                log["b1", u, n].wait_recv()
                u1[u, n] = t2[u, blk] + f3[u, n]
                if n == 1:
                    log["b2", u] = send(u1.at[u, 1], f4.at[u], s4.at[u], r4.at[u], at(ax, p2(pos)))

    lane = lax.broadcasted_iota(jnp.int32, (8, 128), 1)

    def finish(c):
        parts = []
        for u in units(c):
            log["b2", u].wait_recv()
            parts.append(u1[u, 0] + f4[u])
        for m in range(3):
            v = jnp.concatenate([parts[j][m] for j in range(3)], axis=1)
            for k in range(4):
                w = v if k == 0 else pltpu.roll(v, 384 - 96 * k, 1)
                zbuf[32 * c + 8 * k:32 * c + 8 * k + 8, 128 * m:128 * m + 128] = jnp.where(lane < 96, w[:, :128], 0.0)

    with jax.named_scope("first_phase"):
        lax.fori_loop(0, NB, first_phase, 0)
    with jax.named_scope("chunk0"):
        second_phase(0, 0, 8)
    with jax.named_scope("barrier"):
        pl.semaphore_wait(barrier, 38)
    start_pair(0)
    gs = [send(g.at[5], gr.at[0], sg.at[0], rg.at[0], dev(pool, (slab + 1) % 16)),
          send(g.at[0], gr.at[1], sg.at[1], rg.at[1], dev(pool, (slab + 15) % 16))]
    with jax.named_scope("chunk1a"):
        second_phase(1, 0, 4)
    with jax.named_scope("comm1a"):
        start_a1(0)
    with jax.named_scope("chunk1b"):
        second_phase(1, 4, 8)
    with jax.named_scope("comm1b"):
        start_pair(1)
        start_a2(0)
    with jax.named_scope("chunk2a"):
        second_phase(2, 0, 4)
    with jax.named_scope("comm2a"):
        start_a1(1)
        start_b1(0)
    with jax.named_scope("chunk2b"):
        second_phase(2, 4, 8)
    with jax.named_scope("comm2b"):
        start_pair(2)
        start_a2(1)
        start_b2(0)
    with jax.named_scope("tail_a1"):
        start_a1(2)
        start_b1(1)
        finish(0)
    with jax.named_scope("tail_a2"):
        start_a2(2)
        start_b2(1)
    with jax.named_scope("tail_b1"):
        start_b1(2)
        finish(1)
    with jax.named_scope("tail_b2"):
        start_b2(2)
    with jax.named_scope("tail_end"):
        finish(2)

    with jax.named_scope("solve"):
        zk = zbuf[...]
        vh = exact(hz[...], zk)
        kz = lax.broadcasted_iota(jnp.int32, (96, 128), 0)
        ky = lax.broadcasted_iota(jnp.int32, (96, 128), 1)
        qz = jnp.where(2 * kz >= N, kz - N, kz)
        qy = jnp.where(2 * ky >= N, ky - N, ky)
        zy = qz * qz + qy * qy
        scaled = []
        for m in range(3):
            kx = jnp.full((96, 128), 1, jnp.int32) * (3 * (core * 16 + pool) + m)
            qx = jnp.where(2 * kx >= N, kx - N, kx)
            squared = (zy + qx * qx).astype(f32) * ((full_turn / N) ** 2)
            screen = jnp.where(squared > 0, full_turn / jnp.where(squared > 0, squared, 1.0), 0.0)
            scaled.append(vh[:, 128 * m:128 * m + 128] * screen)
        vz = exact(hze[...], jnp.concatenate(scaled, axis=1))
        rz_ = exact(sel[...], zk)
        rows = jnp.concatenate([v[:, 128 * m:128 * m + 128] for v in (rz_, vz) for m in range(3)], axis=0)
        both = exact(rows, hye[...])
        for n in range(6):
            for zd in range(8):
                zs[zd, n] = both[128 * n + 16 * zd:128 * n + 16 * zd + 16]

    with jax.named_scope("zstage"):
        def col(k):
            return dev(pool, ((zc + k) % 8) * 2 + core)
        relay = send(zs.at[(zc + 4) % 8], zrel.at[0], sz.at[0], rz.at[0], col(7))
        zcp = [send(zs.at[(zc + k) % 8], zr.at[k - 1], sz.at[k], rz.at[k], col(k)) for k in (3, 6, 2, 7, 1)]
        relay.wait_recv()
        zrel[1] = zs[(zc + 5) % 8] + zrel[0]
        zcp.append(send(zrel.at[1], zr.at[4], sz.at[5], rz.at[5], col(5)))
        f = zs[zc]
        for cp, k in zip(reversed(zcp[:-1]), (1, 7, 2, 6, 3)):
            cp.wait_recv()
            f = f + zr[k - 1]
        zcp[-1].wait_recv()
        f = f + zr[4]

    with jax.named_scope("rows_out"):
        for c2 in range(2):
            for m in range(3):
                base = c2 * 128 + m
                q[pl.ds(base, 10, stride=8), :] = f[m][6 * c2:6 * c2 + 10]
                q[pl.ds(base + 80, 6, stride=8), :] = f[3 + m][6 * c2 + 2:6 * c2 + 8]
        me = core * 16 + pool

        def row(c2, p2):
            return pl.ds(pl.multiple_of((c2 * 16 + p2) * 8, 8), 8)
        mine = pl.ds(pl.multiple_of(me * 8, 8), 8)
        acp = []
        for k in range(1, 32):
            c2, p2, who = plane(k)
            acp.append(send(q.at[row(c2, p2)], a.at[mine], sa.at[k - 1], ra.at[k - 1], who))
        a[mine, :] = q[row(core, pool), :]
        for cp in acp:
            cp.wait_recv()
    with jax.named_scope("rows_back"):
        hi, lo = halves(a[...])
        xo[...] = jnp.dot(hxe[...], jnp.concatenate([hi, lo, hi], axis=0), preferred_element_type=f32).reshape(16, 16, 128)
        bcp = []
        for k in range(1, 16):
            p2 = (pool + k) % 16
            bcp.append(send(xo.at[p2], b.at[pool], sb.at[k - 1], rb.at[k - 1], dev(p2, slab)))
        b[pool] = xo[pool]
        for cp in gs:
            cp.wait_recv()
        for cp in bcp:
            cp.wait_recv()

    with jax.named_scope("final"):
        def up(v, ax):
            return pltpu.roll(v, v.shape[ax] - 1, ax)

        def down(v, ax):
            return pltpu.roll(v, 1, ax)
        flux = []
        for n in range(8):
            coef = gr[0] if n == 0 else gr[1] if n == 7 else g[n - 1]
            flux.append(coef * ((b[n + 2] - b[n]) * 0.5))
        for n in range(6):
            rho, coef = b[n + 2], g[n]
            div = (flux[n + 2] - flux[n]) * 0.5
            for ax in (0, 1):
                slope = coef * ((up(rho, ax) - down(rho, ax)) * 0.5)
                div = div + (up(slope, ax) - down(slope, ax)) * 0.5
            out[n] = b[10 + n] + l[n] * rho - div

    for cp in [*log.values(), *gs, relay, *zcp, *acp, *bcp]:
        cp.wait_send()


def run(wave, resp, occ, idx, g, l):
    t, hu = np_tables()
    f32, bf = jnp.float32, jnp.bfloat16
    consts = [jnp.asarray(v, bf) for v in (t, *y_tables(t), dense_tables(hu), np.concatenate([hu, hu], axis=1))]
    consts += [jnp.asarray(v, f32) for v in window_tables(hu)]
    consts.append(jnp.asarray(x_table(hu), bf))
    vm, sm, hbm = (pl.BlockSpec(memory_space=m) for m in (pltpu.VMEM, pltpu.SMEM, pl.ANY))
    dma = pltpu.SemaphoreType.DMA
    buf = lambda *dims: pltpu.VMEM(dims, f32)
    return pl.pallas_call(
        kernel,
        out_shape=jax.ShapeDtypeStruct((6, 16, 128), f32),
        in_specs=[sm, sm, hbm, hbm, vm, vm] + [vm] * len(consts),
        out_specs=vm,
        scratch_shapes=[
            pltpu.VMEM((NB, 2, 96, BL), bf), pltpu.VMEM((NB, 2, 96, BL), bf),
            buf(2, 9216, 128), buf(2, 9216, 128), buf(9, 768, 128), buf(9, 384, 128), buf(9, 4, 4, 3, 8, 128),
            buf(9, 2, 4, 3, 8, 128), buf(9, 2, 4, 3, 8, 128), buf(9, 4, 3, 8, 128), buf(9, 4, 3, 8, 128),
            buf(9, 2, 3, 8, 128), buf(9, 2, 3, 8, 128), buf(9, 3, 8, 128), buf(96, 384),
            buf(8, 6, 16, 128), buf(2, 6, 16, 128), buf(7, 6, 16, 128), buf(256, 128), buf(256, 128),
            buf(16, 16, 128), buf(16, 16, 128), buf(2, 16, 128),
            dma((2, NB)), dma((9,)), dma((9,)), dma((9, 2)), dma((9, 2)), dma((9,)), dma((9,)), dma((9, 2)), dma((9, 2)),
            dma((9,)), dma((9,)), dma((8,)), dma((8,)), dma((31,)), dma((31,)), dma((15,)), dma((15,)), dma((2,)), dma((2,)),
        ],
        compiler_params=pltpu.CompilerParams(collective_id=0, has_side_effects=True, vmem_limit_bytes=60 * 1024 * 1024),
        name="response",
    )(occ, idx, wave, resp, g, l, *consts)


def rows_of(flat, first):
    grid = flat.reshape(6, N, N)
    wide = jnp.concatenate([grid[:, 94:], grid, grid[:, :10]], axis=1)
    part = lax.dynamic_slice_in_dim(wide, first, 16, 1)
    return jnp.concatenate([part[..., 80:], part, part[..., :16]], axis=2)


def shards(wave_coeff, response_coeff, band_index, occupation, local_kernel, gradient_kernel):
    row = 6 * lax.axis_index("pool")
    res = run(wave_coeff, response_coeff, occupation, band_index, rows_of(gradient_kernel, row), rows_of(local_kernel, row))
    return res[:, 2:8, 16:112].reshape(6, 576)


def solution(mesh):
    return jax.shard_map(
        shards,
        mesh=mesh,
        in_specs=(
            P(("pool", "slab"), None, None, None),
            P(("pool", "slab"), None, None, None),
            P(("pool", "slab")),
            P(),
            P("slab", None),
            P("slab", None),
        ),
        out_specs=P("slab", "pool"),
        check_vma=False,
    )
```

```python
import math

import numpy as np
import jax
import jax.numpy as jnp
from jax import lax
from jax.experimental import pallas as pl
from jax.experimental.pallas import tpu as pltpu
from jax.sharding import PartitionSpec as P

MESH = pl.DeviceIdType.MESH
full_turn = 2.0 * math.pi
N = 96
BL = 1536
NB = 9216 // BL
STEP = 97


def np_tables():
    k = np.arange(N)
    ang = (np.outer(k, k) % N) * (2 * np.pi / N)
    c, s = np.cos(ang) / np.sqrt(N), np.sin(ang) / np.sqrt(N)
    t = np.block([[c, -s], [s, c]])
    return t, np.cos(ang) + np.sin(ang)


def y_tables(t):
    outs = []
    for row in range(4):
        js = sorted({(96 * row) // 128, (96 * row + 95) // 128})
        w = np.zeros((256 * len(js), 256))
        for n, j in enumerate(js):
            for l in range(128):
                d = 128 * j + l
                if d // 96 != row:
                    continue
                for s in range(2):
                    for r in range(2):
                        w[256 * n + 128 * s + l, 128 * r:128 * r + 96] = t[96 * r:96 * r + 96, 96 * s + d % 96]
        outs.append(w)
    return outs


def dense_tables(hu):
    outs = []
    for j in range(3):
        w = np.zeros((256, 128))
        for l in range(128):
            q, ky = divmod(128 * j + l, 96)
            w[(q - j) * 128:(q - j) * 128 + 96, l] = hu[ky]
        outs.append(np.concatenate([w, w], axis=0))
    return np.stack(outs)


def window_tables(hu):
    h = hu / math.sqrt(N)
    rows = np.array([(12 * zc - 2 + w) % N for zc in range(8) for w in range(16)])
    sel = np.zeros((128, N))
    sel[np.arange(128), rows] = 1.0
    hye = np.zeros((128, 128))
    hye[:N] = hu[:, (np.arange(128) - 16) % N] / N
    return [h, h[rows], sel, hye]


def x_table(hu):
    w = np.zeros((16, 16, 32, 8))
    for p in range(16):
        for i in range(10):
            w[p, i, :, :3] = (hu[(6 * p - 2 + i) % N] / N).reshape(32, 3)
    w = w.reshape(256, 256)
    hi = w.astype(jnp.bfloat16).astype(np.float64)
    return np.concatenate([hi, hi, w - hi], axis=1)


def exact(a, b):
    return jnp.dot(a, b, precision=lax.Precision.HIGHEST, preferred_element_type=jnp.float32)


def halves(v):
    hi = v.astype(jnp.bfloat16)
    return hi, (v - hi.astype(jnp.float32)).astype(jnp.bfloat16)


def swap(t):
    return t + 1 - 2 * (t % 2)


def mirror(t):
    return 3 - t


def kernel(occ, idx, wave, resp, grad, local, *refs):
    tables, out, held, refs = refs[:12], refs[12], refs[13:25], refs[25:]
    (cw, cr, bw, br, d, pbuf, s, f1, t1, f2, t2, f3, zbuf, zs, zr, q, a, xo, b, gr, flat, gl, pot,
     csem, tsem, gsem, p_snd, p_rcv, s1, r1, s2, r2, s3, r3, sz, rz, sa, ra, sb, rb, sg, rg) = refs
    t_ref, w0, w1, w2, w3, yd, hx, hz, hze, sel, hye, hxe = held
    f32, bf = jnp.float32, jnp.bfloat16
    pool, slab = lax.axis_index("pool"), lax.axis_index("slab")
    y, x = pool // 4, pool % 4
    zc, core = slab // 2, slab % 2
    other = 1 - core

    def load(k, blk):
        return pltpu.make_async_copy((wave, resp)[k].at[0, :, :, pl.ds(pl.multiple_of(blk * BL, BL), BL)], (cw, cr)[k].at[blk], csem.at[k, blk])

    early = [pltpu.make_async_copy(tables[n], held[n], tsem.at[n]) for n in range(5)]
    late = [pltpu.make_async_copy(tables[n], held[n], tsem.at[n]) for n in range(5, 12)]
    for cp in early:
        cp.start()
    for blk in range(NB):
        for k in range(2):
            load(k, blk).start()
    for cp in late:
        cp.start()
    grids = []
    for k, src in enumerate((grad, local)):
        for n, (lo, to, size) in enumerate(((0, 384, 9216), (9216 - 384, 0, 384), (0, 9600, 384))):
            grids.append(pltpu.make_async_copy(src.at[:, pl.ds(lo, size)], flat.at[k, :, pl.ds(to, size)], gsem.at[k, n]))
            grids[-1].start()

    def dev(p, sl):
        return {"pool": p, "slab": sl}

    def plane(k):
        dc, dp = k // 16, k % 16
        c2 = (core + dc) % 2
        p2 = (pool + dp) % 16
        return c2, p2, dev(p2, zc * 2 + c2)

    barrier = pltpu.get_barrier_semaphore()

    def hail(who):
        pl.semaphore_signal(barrier, inc=1, device_id=who, device_id_type=MESH)

    for k in range(1, 32):
        hail(plane(k)[2])
    for dz in range(1, 8):
        hail(dev(pool, (slab + 2 * dz) % 16))
    hail(dev(pool, (slab + 15 + 2 * core) % 16))

    def send(src, dst, ssem, rsem, who):
        cp = pltpu.make_async_remote_copy(src_ref=src, dst_ref=dst, send_sem=ssem, recv_sem=rsem, device_id=who, device_id_type=MESH)
        cp.start()
        return cp

    q[...] = jnp.zeros_like(q)
    for u in range(9):
        d[u, pl.ds(8, 96, stride=9), :] = jnp.zeros((96, 128), f32)
    for cp in early:
        cp.wait()

    def first_phase(blk, carry):
        for k in range(2):
            load(k, blk).wait()
        t = t_ref[...]
        for src, dst in ((cw, bw), (cr, br)):
            c = jnp.concatenate([src[blk, 0], src[blk, 1]], axis=0)
            zb = jnp.dot(t, c, preferred_element_type=f32).astype(bf)
            groups = BL // 384
            for row, w in enumerate((w0, w1, w2, w3)):
                js = sorted({(96 * row) // 128, (96 * row + 95) // 128})
                lhs = jnp.concatenate([
                    jnp.concatenate([zb[96 * r:96 * r + 96, 384 * n + 128 * j:384 * n + 128 * j + 128] for j in js for r in range(2)], axis=1)
                    for n in range(groups)], axis=0)
                res = jnp.dot(lhs, w[...], preferred_element_type=f32)
                for n in range(groups):
                    base = (blk * (BL // 96) + 4 * n + row) * STEP
                    for r in range(2):
                        dst[r, pl.ds(base, 96), :] = res[96 * n:96 * n + 96, 128 * r:128 * r + 128]
        return carry

    weight = occ[idx[0]].astype(f32) * (1.0 / 256.0)

    def second_phase(chunk, first, last):
        def body(step, carry):
            t = t_ref[...]
            his, los = [], []
            for n in range(2):
                i = 2 * step + n
                spaces = []
                for src in (bw, br):
                    parts = []
                    for k in range(4):
                        z = chunk * 32 + 8 * k + i
                        parts.append(jnp.concatenate([src[r, pl.ds(z, 96, stride=STEP), :].astype(bf) for r in range(2)], axis=0))
                    spaces.append(jnp.dot(t, jnp.concatenate(parts, axis=1), preferred_element_type=f32))
                v, w = spaces
                hi, lo = halves((v[:96] * w[:96] + v[96:] * w[96:]) * weight)
                his.append(hi)
                los.append(lo)
            hi, lo = jnp.concatenate(his, axis=0), jnp.concatenate(los, axis=0)
            cols = []
            for j in range(3):
                lhs = jnp.concatenate([hi[:, 128 * j:128 * j + 256], lo[:, 128 * j:128 * j + 256]], axis=1)
                cols.append(jnp.dot(lhs, yd[j], preferred_element_type=f32))
            cols = jnp.concatenate([col[96 * n:96 * n + 96] for n in range(2) for col in cols], axis=1)
            gx = jnp.dot(hx[...], jnp.concatenate(halves(cols), axis=0), preferred_element_type=f32)
            for n in range(2):
                for j in range(3):
                    d[3 * chunk + j, pl.ds(2 * step + n, 96, stride=9), :] = gx[:, 384 * n + 128 * j:384 * n + 128 * j + 128]
            return carry
        lax.fori_loop(first, last, body, 0)

    log = {}

    def variant(u):
        return (u % 4) % 2, (u % 4) // 2

    def order(u, along):
        ax, par = variant(u)
        pos = (x, y)[(ax + along) % 2]
        p1, p2 = (swap, mirror) if par == 0 else (mirror, swap)
        return pos, p1, p2, (ax + along) % 2

    def at(ax, pos):
        return dev(y * 4 + pos, slab) if ax == 0 else dev(pos * 4 + x, slab)

    def units(c):
        return range(3 * c, 3 * c + 3)

    def start_pair(c):
        for u in units(c):
            log["p", u] = send(d.at[u, pl.ds(pl.multiple_of(other * 432, 432), 432)], pbuf.at[u], p_snd.at[u], p_rcv.at[u], dev(pool, zc * 2 + other))

    def start_a1(c):
        for u in units(c):
            log["p", u].wait_recv()
            for n in range(48):
                s[u, n // 12, n // 3 % 4, n % 3] = d[u, pl.ds(core * 432 + 9 * n, 8), :] + pbuf[u, pl.ds(9 * n, 8), :]
            pos, p1, p2, ax = order(u, 0)
            to = p1(pos)
            for n, blk in enumerate((to, p2(to))):
                src = s.at[u, :, blk] if ax == 0 else s.at[u, blk]
                log["a1", u, n] = send(src, f1.at[u, n], s1.at[u, n], r1.at[u, n], at(ax, to))

    def start_a2(c):
        for u in units(c):
            pos, p1, p2, ax = order(u, 0)
            for n, blk in ((1, p2(pos)), (0, pos)):
                log["a1", u, n].wait_recv()
                own = s[u, :, blk] if ax == 0 else s[u, blk]
                t1[u, n] = own + f1[u, n]
                if n == 1:
                    log["a2", u] = send(t1.at[u, 1], f2.at[u], s2.at[u], r2.at[u], at(ax, p2(pos)))

    def start_b(c):
        for u in units(c):
            log["a2", u].wait_recv()
            t2[u] = t1[u, 0] + f2[u]
            pos, _, _, ax = order(u, 1)
            for k in (2, 1, 3):
                to = (pos + k) % 4
                log["b", u, k] = send(t2.at[u, to], f3.at[u, k - 1], s3.at[u, k - 1], r3.at[u, k - 1], at(ax, to))

    lane = lax.broadcasted_iota(jnp.int32, (8, 128), 1)

    def finish(c):
        parts = []
        for u in units(c):
            part = t2[u, order(u, 1)[0]]
            for k in (1, 3, 2):
                log["b", u, k].wait_recv()
                part = part + f3[u, k - 1]
            parts.append(part)
        for m in range(3):
            v = jnp.concatenate([parts[j][m] for j in range(3)], axis=1)
            for k in range(4):
                w = v if k == 0 else pltpu.roll(v, 384 - 96 * k, 1)
                zbuf[32 * c + 8 * k:32 * c + 8 * k + 8, 128 * m:128 * m + 128] = jnp.where(lane < 96, w[:, :128], 0.0)

    with jax.named_scope("first_phase"):
        lax.fori_loop(0, NB, first_phase, 0)
    with jax.named_scope("chunk0"):
        for cp in late:
            cp.wait()
        second_phase(0, 0, 4)
    with jax.named_scope("barrier"):
        pl.semaphore_wait(barrier, 39)
    start_pair(0)
    with jax.named_scope("chunk1a"):
        second_phase(1, 0, 2)
    with jax.named_scope("comm1a"):
        start_a1(0)
    with jax.named_scope("chunk1b"):
        second_phase(1, 2, 4)
    with jax.named_scope("comm1b"):
        start_pair(1)
        start_a2(0)
    with jax.named_scope("chunk2a"):
        second_phase(2, 0, 2)
    with jax.named_scope("comm2a"):
        start_a1(1)
        start_b(0)
    with jax.named_scope("chunk2b"):
        second_phase(2, 2, 4)
    with jax.named_scope("comm2b"):
        start_pair(2)
        start_a2(1)
        finish(0)
    with jax.named_scope("tail_a1"):
        start_a1(2)
        start_b(1)
    with jax.named_scope("tail_a2"):
        start_a2(2)
        finish(1)
    with jax.named_scope("tail_b"):
        start_b(2)
    with jax.named_scope("tail_end"):
        finish(2)

    with jax.named_scope("solve"):
        zk = zbuf[...]
        vh = exact(hz[...], zk)
        kz = lax.broadcasted_iota(jnp.int32, (96, 128), 0)
        ky = lax.broadcasted_iota(jnp.int32, (96, 128), 1)
        qz = jnp.where(2 * kz >= N, kz - N, kz)
        qy = jnp.where(2 * ky >= N, ky - N, ky)
        zy = qz * qz + qy * qy
        scaled = []
        for m in range(3):
            kx = jnp.full((96, 128), 1, jnp.int32) * (3 * (core * 16 + pool) + m)
            qx = jnp.where(2 * kx >= N, kx - N, kx)
            squared = (zy + qx * qx).astype(f32) * ((full_turn / N) ** 2)
            screen = jnp.where(squared > 0, full_turn / jnp.where(squared > 0, squared, 1.0), 0.0)
            scaled.append(vh[:, 128 * m:128 * m + 128] * screen)
        vz = exact(hze[...], jnp.concatenate(scaled, axis=1))
        rz_ = exact(sel[...], zk)
        rows = jnp.concatenate([v[:, 128 * m:128 * m + 128] for v in (rz_, vz) for m in range(3)], axis=0)
        both = exact(rows, hye[...])
        for n in range(6):
            for zd in range(8):
                zs[zd, n] = both[128 * n + 16 * zd:128 * n + 16 * zd + 16]

    with jax.named_scope("zstage"):
        def col(k):
            return dev(pool, ((zc + k) % 8) * 2 + core)
        zcp = [(k, send(zs.at[(zc + k) % 8], zr.at[k - 1], sz.at[k], rz.at[k], col(k))) for k in (4, 3, 5, 2, 6, 1, 7)]
        for cp in grids:
            cp.wait()
        odd = pool % 2
        wide = lax.broadcasted_iota(jnp.int32, (6, 128), 1)
        for k in range(2):
            v = flat[k, :, pl.ds(pl.multiple_of(576 * pool - 64 * odd, 128), 1408)]
            v = jnp.where(odd == 1, pltpu.roll(v, 1408 - 64, 1), v)
            wins = [v[:, 176 + 96 * w:304 + 96 * w] for w in range(-1, 11)]
            for w in range(10):
                gl[k, pl.ds(w, 6, stride=16), :] = jnp.where(wide < 16, wins[w + 2], jnp.where(wide >= 112, wins[w], wins[w + 1]))
        gs = [send(gl.at[0, pl.ds(80, 16)], gr.at[0], sg.at[0], rg.at[0], dev(pool, (slab + 1) % 16)),
              send(gl.at[0, pl.ds(0, 16)], gr.at[1], sg.at[1], rg.at[1], dev(pool, (slab + 15) % 16))]
        f = zs[zc]
        for k, cp in reversed(zcp):
            cp.wait_recv()
            f = f + zr[k - 1]

    with jax.named_scope("rows_out"):
        for c2 in range(2):
            for m in range(3):
                base = c2 * 128 + m
                q[pl.ds(base, 10, stride=8), :] = f[m][6 * c2:6 * c2 + 10]
                q[pl.ds(base + 80, 6, stride=8), :] = f[3 + m][6 * c2 + 2:6 * c2 + 8]
        me = core * 16 + pool

        def row(c2, p2):
            return pl.ds(pl.multiple_of((c2 * 16 + p2) * 8, 8), 8)
        mine = pl.ds(pl.multiple_of(me * 8, 8), 8)
        acp = []
        for k in range(1, 32):
            c2, p2, who = plane(k)
            acp.append(send(q.at[row(c2, p2)], a.at[mine], sa.at[k - 1], ra.at[k - 1], who))
        a[mine, :] = q[row(core, pool), :]
        for cp in acp:
            cp.wait_recv()
    with jax.named_scope("rows_back"):
        hi, lo = halves(a[...])
        xo[...] = jnp.dot(hxe[...], jnp.concatenate([hi, lo, hi], axis=0), preferred_element_type=f32).reshape(16, 16, 128)
        bcp = []
        for k in range(1, 16):
            p2 = (pool + k) % 16
            bcp.append(send(xo.at[p2], b.at[pool], sb.at[k - 1], rb.at[k - 1], dev(p2, slab)))
        b[pool] = xo[pool]
        for cp in gs:
            cp.wait_recv()
        for cp in bcp:
            cp.wait_recv()

    with jax.named_scope("final"):
        def up(v, ax):
            return pltpu.roll(v, v.shape[ax] - 1, ax)

        def down(v, ax):
            return pltpu.roll(v, 1, ax)
        g = [gl[0, pl.ds(16 * n, 16), :] for n in range(6)]
        flux = []
        for n in range(8):
            coef = gr[0] if n == 0 else gr[1] if n == 7 else g[n - 1]
            flux.append(coef * ((b[n + 2] - b[n]) * 0.5))
        for n in range(6):
            rho, coef = b[n + 2], g[n]
            div = (flux[n + 2] - flux[n]) * 0.5
            for ax in (0, 1):
                slope = coef * ((up(rho, ax) - down(rho, ax)) * 0.5)
                div = div + (up(slope, ax) - down(slope, ax)) * 0.5
            pot[pl.ds(16 * n, 16), :] = b[10 + n] + gl[1, pl.ds(16 * n, 16), :] * rho - div
        row640 = lax.broadcasted_iota(jnp.int32, (6, 640), 1)
        whole = jnp.zeros((6, 640), f32)
        for w in range(6):
            piece = jnp.concatenate([pot[pl.ds(w + 2, 6, stride=16), :], jnp.zeros((6, 512), f32)], axis=1)
            piece = pltpu.roll(piece, (96 * w - 16) % 640, 1)
            whole = jnp.where((row640 >= 96 * w) & (row640 < 96 * w + 96), piece, whole)
        out[...] = whole[:, :576]

    for cp in [*log.values(), *gs, *(cp for _, cp in zcp), *acp, *bcp]:
        cp.wait_send()


def run(wave, resp, occ, idx, grad, local):
    t, hu = np_tables()
    f32, bf = jnp.float32, jnp.bfloat16
    consts = [jnp.asarray(v, bf) for v in (t, *y_tables(t), dense_tables(hu), np.concatenate([hu, hu], axis=1))]
    consts += [jnp.asarray(v, f32) for v in window_tables(hu)]
    consts.append(jnp.asarray(x_table(hu), bf))
    vm, sm, hbm = (pl.BlockSpec(memory_space=m) for m in (pltpu.VMEM, pltpu.SMEM, pl.ANY))
    dma = pltpu.SemaphoreType.DMA
    buf = lambda *dims: pltpu.VMEM(dims, f32)
    return pl.pallas_call(
        kernel,
        out_shape=jax.ShapeDtypeStruct((6, 576), f32),
        in_specs=[sm, sm, hbm, hbm, hbm, hbm] + [hbm] * len(consts),
        out_specs=vm,
        scratch_shapes=[
            *(pltpu.VMEM(v.shape, v.dtype) for v in consts),
            pltpu.VMEM((NB, 2, 96, BL), bf), pltpu.VMEM((NB, 2, 96, BL), bf),
            buf(2, 96 * STEP, 128), buf(2, 96 * STEP, 128), buf(9, 864, 128), buf(9, 432, 128), buf(9, 4, 4, 3, 8, 128),
            buf(9, 2, 4, 3, 8, 128), buf(9, 2, 4, 3, 8, 128), buf(9, 4, 3, 8, 128), buf(9, 4, 3, 8, 128),
            buf(9, 3, 3, 8, 128), buf(96, 384), buf(8, 6, 16, 128), buf(7, 6, 16, 128), buf(256, 128), buf(256, 128),
            buf(16, 16, 128), buf(16, 16, 128), buf(2, 16, 128), buf(2, 6, 9984), buf(2, 96, 128), buf(96, 128),
            dma((2, NB)), dma((12,)), dma((2, 3)), dma((9,)), dma((9,)), dma((9, 2)), dma((9, 2)), dma((9,)), dma((9,)), dma((9, 3)), dma((9, 3)),
            dma((8,)), dma((8,)), dma((31,)), dma((31,)), dma((15,)), dma((15,)), dma((2,)), dma((2,)),
        ],
        compiler_params=pltpu.CompilerParams(collective_id=0, has_side_effects=True, vmem_limit_bytes=60 * 1024 * 1024),
        name="response",
    )(occ, idx, wave, resp, grad, local, *consts)


def shards(wave_coeff, response_coeff, band_index, occupation, local_kernel, gradient_kernel):
    return run(wave_coeff, response_coeff, occupation, band_index, gradient_kernel, local_kernel)


def solution(mesh):
    return jax.shard_map(
        shards,
        mesh=mesh,
        in_specs=(
            P(("pool", "slab"), None, None, None),
            P(("pool", "slab"), None, None, None),
            P(("pool", "slab")),
            P(),
            P("slab", None),
            P("slab", None),
        ),
        out_specs=P("slab", "pool"),
        check_vma=False,
    )
```

```python
import math

import numpy as np
import jax
import jax.numpy as jnp
from jax import lax
from jax.experimental import pallas as pl
from jax.experimental.pallas import tpu as pltpu
from jax.sharding import PartitionSpec as P

MESH = pl.DeviceIdType.MESH
full_turn = 2.0 * math.pi
N = 96
BL = 1536
NB = 9216 // BL
STEP = 97


def np_tables():
    k = np.arange(N)
    ang = (np.outer(k, k) % N) * (2 * np.pi / N)
    c, s = np.cos(ang) / np.sqrt(N), np.sin(ang) / np.sqrt(N)
    t = np.block([[c, -s], [s, c]])
    return t, np.cos(ang) + np.sin(ang)


def y_tables(t):
    outs = []
    for row in range(4):
        js = sorted({(96 * row) // 128, (96 * row + 95) // 128})
        w = np.zeros((256 * len(js), 256))
        for n, j in enumerate(js):
            for l in range(128):
                d = 128 * j + l
                if d // 96 != row:
                    continue
                for s in range(2):
                    for r in range(2):
                        w[256 * n + 128 * s + l, 128 * r:128 * r + 96] = t[96 * r:96 * r + 96, 96 * s + d % 96]
        outs.append(w)
    return outs


def dense_tables(hu):
    outs = []
    for j in range(3):
        w = np.zeros((256, 128))
        for l in range(128):
            q, ky = divmod(128 * j + l, 96)
            w[(q - j) * 128:(q - j) * 128 + 96, l] = hu[ky]
        outs.append(np.concatenate([w, w], axis=0))
    return np.stack(outs)


def inverse_tables(hu):
    hye = np.zeros((128, 128))
    hye[:N] = hu[:, (np.arange(128) - 16) % N] / N
    return [hu / math.sqrt(N), hye]


def x_table(hu):
    w = np.zeros((16, 16, 32, 8))
    for p in range(16):
        for i in range(10):
            w[p, i, :, :3] = (hu[(6 * p - 2 + i) % N] / N).reshape(32, 3)
    w = w.reshape(256, 256)
    hi = w.astype(jnp.bfloat16).astype(np.float64)
    return np.concatenate([hi, hi, w - hi], axis=1)


def exact(a, b):
    return jnp.dot(a, b, precision=lax.Precision.HIGHEST, preferred_element_type=jnp.float32)


def halves(v):
    hi = v.astype(jnp.bfloat16)
    return hi, (v - hi.astype(jnp.float32)).astype(jnp.bfloat16)


def swap(t):
    return t + 1 - 2 * (t % 2)


def mirror(t):
    return 3 - t


def kernel(occupation, numbers, wave, resp, grad, local, *refs):
    tables, out, held, refs = refs[:7], refs[7], refs[8:15], refs[15:]
    (occ, idx, cc, bw, br, d, pbuf, s, f1, t2, f3, zbuf, rbuf, zp, zpr, zv, zvr, q, a, xo, b, gr, flat, gl, pot,
     csem, tsem, gsem, osem, p_snd, p_rcv, s1, r1, s3, r3, sp, rp, sv, rv, sa, ra, sb, rb, sg, rg) = refs
    t_ref, wy, yd, hx, hz, hye, hxe = held
    f32, bf = jnp.float32, jnp.bfloat16
    pool, slab = lax.axis_index("pool"), lax.axis_index("slab")
    y, x = pool // 4, pool % 4
    zc, core = slab // 2, slab % 2
    other = 1 - core

    def load(k, blk):
        return pltpu.make_async_copy((wave, resp)[k].at[0, :, :, pl.ds(blk * BL, BL)], cc.at[blk, k], csem.at[blk])

    early = [pltpu.make_async_copy(tables[n], held[n], tsem.at[n]) for n in range(2)]
    late = [pltpu.make_async_copy(tables[n], held[n], tsem.at[n]) for n in range(2, 7)]
    for cp in early:
        cp.start()
    for blk in range(NB):
        for k in range(2):
            load(k, blk).start()
    for cp in late:
        cp.start()
    weights = [pltpu.make_async_copy(occupation, occ, osem.at[0]), pltpu.make_async_copy(numbers, idx, osem.at[1])]
    for cp in weights:
        cp.start()
    for k, src in enumerate((grad, local)):
        for lo, to, size in ((0, 384, 9216), (9216 - 384, 0, 384), (0, 9600, 384)):
            pltpu.make_async_copy(src.at[:, pl.ds(lo, size)], flat.at[k, :, pl.ds(to, size)], gsem.at[0]).start()

    def drain(ref, sem):
        pltpu.make_async_copy(ref, ref, sem).wait()


    def dev(p, sl):
        return {"pool": p, "slab": sl}

    def plane(k):
        dc, dp = k // 16, k % 16
        c2 = (core + dc) % 2
        p2 = (pool + dp) % 16
        return c2, p2, dev(p2, zc * 2 + c2)

    barrier = pltpu.get_barrier_semaphore()

    def hail(who):
        pl.semaphore_signal(barrier, inc=1, device_id=who, device_id_type=MESH)

    for k in range(1, 32):
        hail(plane(k)[2])
    for dz in range(1, 8):
        hail(dev(pool, (slab + 2 * dz) % 16))
    hail(dev(pool, (slab + 15 + 2 * core) % 16))
    for r in range(12, 16):
        hail(dev(r, (slab + (1 if r < 14 else 15)) % 16))

    def send(src, dst, ssem, rsem, who):
        cp = pltpu.make_async_remote_copy(src_ref=src, dst_ref=dst, send_sem=ssem, recv_sem=rsem, device_id=who, device_id_type=MESH)
        cp.start()
        return cp

    for ref in (q, a, b):
        ref[...] = jnp.zeros_like(ref)
    for cp in early:
        cp.wait()

    def first_phase(blk, carry):
        drain(cc.at[blk], csem.at[blk])
        t = t_ref[...]
        for k, dst in enumerate((bw, br)):
            c = jnp.concatenate([cc[blk, k, 0], cc[blk, k, 1]], axis=0)
            zb = jnp.dot(t, c, preferred_element_type=f32).astype(bf)
            groups = BL // 384
            for row, (lo, hi) in enumerate(((0, 256), (256, 768), (768, 1280), (1280, 1536))):
                js = sorted({(96 * row) // 128, (96 * row + 95) // 128})
                lhs = jnp.concatenate([
                    jnp.concatenate([zb[96 * r:96 * r + 96, 384 * n + 128 * j:384 * n + 128 * j + 128] for j in js for r in range(2)], axis=1)
                    for n in range(groups)], axis=0)
                res = jnp.dot(lhs, wy[lo:hi], preferred_element_type=f32)
                for n in range(groups):
                    base = (blk * (BL // 96) + 4 * n + row) * STEP
                    for r in range(2):
                        dst[r, pl.ds(base, 96), :] = res[96 * n:96 * n + 96, 128 * r:128 * r + 128]
        return carry

    def second_phase(chunk, first, last):
        def body(step, carry):
            t = t_ref[...]
            weight = occ[idx[0]].astype(f32) * (1.0 / 256.0)
            his, los = [], []
            for n in range(2):
                i = 2 * step + n
                spaces = []
                for src in (bw, br):
                    parts = []
                    for k in range(4):
                        z = chunk * 32 + 8 * k + i
                        parts.append(jnp.concatenate([src[r, pl.ds(z, 96, stride=STEP), :].astype(bf) for r in range(2)], axis=0))
                    spaces.append(jnp.dot(t, jnp.concatenate(parts, axis=1), preferred_element_type=f32))
                v, w = spaces
                hi, lo = halves((v[:96] * w[:96] + v[96:] * w[96:]) * weight)
                his.append(hi)
                los.append(lo)
            hi, lo = jnp.concatenate(his, axis=0), jnp.concatenate(los, axis=0)
            cols = []
            for j in range(3):
                lhs = jnp.concatenate([hi[:, 128 * j:128 * j + 256], lo[:, 128 * j:128 * j + 256]], axis=1)
                cols.append(jnp.dot(lhs, yd[j], preferred_element_type=f32))
            cols = jnp.concatenate([col[96 * n:96 * n + 96] for n in range(2) for col in cols], axis=1)
            gx = jnp.dot(hx[...], jnp.concatenate(halves(cols), axis=0), preferred_element_type=f32)
            for n in range(2):
                for j in range(3):
                    d[3 * chunk + j, pl.ds(2 * step + n, 96, stride=9), :] = gx[:, 384 * n + 128 * j:384 * n + 128 * j + 128]
            return carry
        lax.fori_loop(first, last, body, 0)


    def order(u, m, along):
        ax = (3 * u + m + along) % 2
        return (x, y)[ax], ax

    def at(ax, pos):
        return dev(y * 4 + pos, slab) if ax == 0 else dev(pos * 4 + x, slab)

    def units(c):
        return range(3 * c, 3 * c + 3)

    def start_pair(c):
        for u in units(c):
            send(d.at[u, pl.ds(pl.multiple_of(other * 432, 432), 432)], pbuf.at[u], p_snd.at[0], p_rcv.at[c], dev(pool, zc * 2 + other))

    def start_a(c):
        drain(pbuf.at[pl.ds(3 * c, 3)], p_rcv.at[c])
        for u in units(c):
            for n in range(48):
                s[u, n // 12, n // 3 % 4, n % 3] = d[u, pl.ds(core * 432 + 9 * n, 8), :] + pbuf[u, pl.ds(9 * n, 8), :]
            for m in range(3):
                pos, ax = order(u, m, 0)
                for k in (2, 1, 3):
                    to = (pos + k) % 4
                    src = s.at[u, :, to, m] if ax == 0 else s.at[u, to, :, m]
                    send(src, f1.at[u, m, k - 1], s1.at[0], r1.at[c], at(ax, to))

    def start_b(c):
        drain(f1.at[pl.ds(3 * c, 3)], r1.at[c])
        for u in units(c):
            for m in range(3):
                pos, ax = order(u, m, 0)
                part = s[u, :, pos, m] if ax == 0 else s[u, pos, :, m]
                for k in (1, 3, 2):
                    part = part + f1[u, m, k - 1]
                t2[u, m] = part
                pos, ax = order(u, m, 1)
                for k in (2, 1, 3):
                    to = (pos + k) % 4
                    send(t2.at[u, m, to], f3.at[u, m, k - 1], s3.at[0], r3.at[c], at(ax, to))

    lane = lax.broadcasted_iota(jnp.int32, (8, 128), 1)

    def finish(c):
        parts = {}
        drain(f3.at[pl.ds(3 * c, 3)], r3.at[c])
        for u in units(c):
            for m in range(3):
                part = t2[u, m, order(u, m, 1)[0]]
                for k in (1, 3, 2):
                    part = part + f3[u, m, k - 1]
                parts[u - 3 * c, m] = part
        for m in range(3):
            v = jnp.concatenate([parts[j, m] for j in range(3)], axis=1)
            for k in range(4):
                w = v if k == 0 else pltpu.roll(v, 384 - 96 * k, 1)
                zbuf[32 * c + 8 * k:32 * c + 8 * k + 8, 128 * m:128 * m + 128] = jnp.where(lane < 96, w[:, :128], 0.0)
        rows = jnp.concatenate([zbuf[32 * c:32 * c + 32, 128 * m:128 * m + 128] for m in range(3)], axis=0)
        both = exact(rows, hye[...])
        for m in range(3):
            rbuf[m, 32 * c:32 * c + 32, :] = both[32 * m:32 * m + 32]
        for zd in ((0, 1), (2, 3, 4), (5, 6, 7))[c]:
            for m in range(3):
                zp[zd, 12 * m:12 * m + 12, :] = rbuf[m, 12 * zd:12 * zd + 12, :]
            slot = (zd - zc + 15) % 8
            cp = pltpu.make_async_remote_copy(src_ref=zp.at[zd], dst_ref=zpr.at[slot], send_sem=sp.at[0], recv_sem=rp.at[0], device_id=dev(pool, 2 * zd + core), device_id_type=MESH)
            pl.when(zc != zd)(cp.start)

    with jax.named_scope("first_phase"):
        lax.fori_loop(0, NB, first_phase, 0)
    with jax.named_scope("chunk0"):
        for cp in late + weights:
            cp.wait()
        second_phase(0, 0, 4)
    with jax.named_scope("barrier"):
        pl.semaphore_wait(barrier, 39 + 16 * (pool // 12))
    start_pair(0)
    with jax.named_scope("chunk1a"):
        second_phase(1, 0, 2)
    with jax.named_scope("comm1a"):
        start_a(0)
    with jax.named_scope("chunk1b"):
        second_phase(1, 2, 4)
    start_pair(1)
    with jax.named_scope("chunk2a"):
        second_phase(2, 0, 2)
    with jax.named_scope("comm2a"):
        start_a(1)
    with jax.named_scope("chunk2b"):
        second_phase(2, 2, 4)
    start_pair(2)
    with jax.named_scope("tail_a2"):
        start_a(2)
    with jax.named_scope("tail_b0"):
        start_b(0)
    with jax.named_scope("tail_b1"):
        start_b(1)
    with jax.named_scope("tail_fin0"):
        finish(0)
    with jax.named_scope("tail_b2"):
        start_b(2)
    with jax.named_scope("tail_fin1"):
        finish(1)
    with jax.named_scope("tail_fin2"):
        finish(2)

    with jax.named_scope("solve"):
        zk = zbuf[...]
        vh = exact(hz[...], zk)
        kz = lax.broadcasted_iota(jnp.int32, (96, 128), 0)
        ky = lax.broadcasted_iota(jnp.int32, (96, 128), 1)
        qz = jnp.where(2 * kz >= N, kz - N, kz)
        qy = jnp.where(2 * ky >= N, ky - N, ky)
        zy = qz * qz + qy * qy
        scaled = []
        for m in range(3):
            kx = jnp.full((96, 128), 1, jnp.int32) * (3 * (core * 16 + pool) + m)
            qx = jnp.where(2 * kx >= N, kx - N, kx)
            squared = (zy + qx * qx).astype(f32) * ((full_turn / N) ** 2)
            screen = jnp.where(squared > 0, full_turn / jnp.where(squared > 0, squared, 1.0), 0.0)
            scaled.append(vh[:, 128 * m:128 * m + 128] * screen)
        vz = exact(hz[...], jnp.concatenate(scaled, axis=1))
        both = exact(jnp.concatenate([vz[:, 128 * m:128 * m + 128] for m in range(3)], axis=0), hye[...])
        for m in range(3):
            for zd in range(8):
                zv[zd, 12 * m:12 * m + 12, :] = both[96 * m + 12 * zd:96 * m + 12 * zd + 12]

    with jax.named_scope("zstage"):
        def col(k):
            return dev(pool, ((zc + k) % 8) * 2 + core)
        for k in (4, 3, 5, 2, 6, 1, 7):
            send(zv.at[(zc + k) % 8], zvr.at[k - 1], sv.at[0], rv.at[0], col(k))
        drain(flat, gsem.at[0])
        odd = pool % 2
        wide = lax.broadcasted_iota(jnp.int32, (6, 128), 1)
        for k in range(2):
            v = flat[k, :, pl.ds(pl.multiple_of(576 * pool - 64 * odd, 128), 1408)]
            v = jnp.where(odd == 1, pltpu.roll(v, 1408 - 64, 1), v)
            wins = [v[:, 176 + 96 * w:304 + 96 * w] for w in range(-1, 11)]
            for w in range(10):
                gl[k, pl.ds(w, 6, stride=16), :] = jnp.where(wide < 16, wins[w + 2], jnp.where(wide >= 112, wins[w], wins[w + 1]))
        send(gl.at[0, pl.ds(80, 16)], gr.at[0], sg.at[0], rg.at[0], dev(pool, (slab + 1) % 16))
        send(gl.at[0, pl.ds(0, 16)], gr.at[1], sg.at[0], rg.at[0], dev(pool, (slab + 15) % 16))

    me = core * 16 + pool
    mine = pl.ds(pl.multiple_of(me * 8, 8), 3)

    def deal(rows):
        for dc in range(2):
            c2 = (core + dc) % 2
            for r in rows:
                src = q.at[pl.ds(pl.multiple_of((c2 * 16 + r) * 8, 8), 3)]
                cp = pltpu.make_async_remote_copy(src_ref=src, dst_ref=a.at[mine], send_sem=sa.at[0], recv_sem=ra.at[0], device_id=dev(r, zc * 2 + c2), device_id_type=MESH)
                if dc:
                    cp.start()
                else:
                    pl.when(pool != r)(cp.start)

    with jax.named_scope("rows_rho"):
        drain(zpr, rp.at[0])
        f = zp[zc]
        for k in range(7):
            f = f + zpr[k]
        for c2 in range(2):
            for m in range(3):
                base = c2 * 128 + m
                rho6 = f[12 * m + 6 * c2:12 * m + 6 * c2 + 6]
                q[pl.ds(base, 6, stride=8), :] = rho6
                q[pl.ds(base + 96, 2, stride=8), :] = rho6[:2]
                q[pl.ds(base + 112, 2, stride=8), :] = rho6[4:]
        deal((0, 1, 2, 3, 4, 5, 12, 13, 14, 15))
    with jax.named_scope("rows_v"):
        drain(zvr, rv.at[0])
        f = zv[zc]
        for k in range(7):
            f = f + zvr[k]
        for c2 in range(2):
            for m in range(3):
                q[pl.ds(c2 * 128 + m + 48, 6, stride=8), :] = f[12 * m + 6 * c2:12 * m + 6 * c2 + 6]
        deal(range(6, 12))
    with jax.named_scope("rows_out"):
        a[mine, :] = q[pl.ds(pl.multiple_of((core * 16 + pool) * 8, 8), 3), :]
        drain(a.at[pl.ds(0, 93)], ra.at[0])
    with jax.named_scope("rows_back"):
        hi, lo = halves(a[...])
        xo[...] = jnp.dot(hxe[...], jnp.concatenate([hi, lo, hi], axis=0), preferred_element_type=f32).reshape(16, 16, 128)
        edge = pool // 12
        aim = (slab + 16 + edge * (2 * (pool // 14) - 1)) % 16
        for k in range(1, 16):
            p2 = (pool + k) % 16
            send(xo.at[p2, pl.ds(0, 10)], b.at[pool, pl.ds(0, 10)], sb.at[0], rb.at[0], dev(p2, aim))

        def across():
            return pltpu.make_async_remote_copy(src_ref=xo.at[pool, pl.ds(0, 10)], dst_ref=b.at[pool, pl.ds(0, 10)], send_sem=sb.at[1], recv_sem=rb.at[1], device_id=dev(pool, aim), device_id_type=MESH)

        @pl.when(edge == 0)
        def _():
            b[pool] = xo[pool]

        @pl.when(edge == 1)
        def _():
            across().start()
            across().wait()
        drain(gr, rg.at[0])
        drain(a.at[pl.ds(0, 150)], rb.at[0])

    with jax.named_scope("final"):
        def up(v, ax):
            return pltpu.roll(v, v.shape[ax] - 1, ax)

        def down(v, ax):
            return pltpu.roll(v, 1, ax)
        g = [gl[0, pl.ds(16 * n, 16), :] for n in range(6)]
        rhos = [b[n] for n in (14, 15, 0, 1, 2, 3, 4, 5, 12, 13)]
        flux = []
        for n in range(8):
            coef = gr[0] if n == 0 else gr[1] if n == 7 else g[n - 1]
            flux.append(coef * ((rhos[n + 2] - rhos[n]) * 0.5))
        for n in range(6):
            rho, coef = rhos[n + 2], g[n]
            div = (flux[n + 2] - flux[n]) * 0.5
            for ax in (0, 1):
                slope = coef * ((up(rho, ax) - down(rho, ax)) * 0.5)
                div = div + (up(slope, ax) - down(slope, ax)) * 0.5
            pot[pl.ds(16 * n, 16), :] = b[6 + n] + gl[1, pl.ds(16 * n, 16), :] * rho - div
        row640 = lax.broadcasted_iota(jnp.int32, (6, 640), 1)
        whole = jnp.zeros((6, 640), f32)
        for w in range(6):
            piece = jnp.concatenate([pot[pl.ds(w + 2, 6, stride=16), :], jnp.zeros((6, 512), f32)], axis=1)
            piece = pltpu.roll(piece, (96 * w - 16) % 640, 1)
            whole = jnp.where((row640 >= 96 * w) & (row640 < 96 * w + 96), piece, whole)
        out[...] = whole[:, :576]

    with jax.named_scope("sent"):
        for ref, sem in ((pbuf, p_snd), (f1, s1), (f3, s3), (zpr, sp), (zvr, sv), (gr, sg), (a.at[pl.ds(0, 93)], sa), (a.at[pl.ds(0, 150)], sb)):
            drain(ref, sem.at[0])


def run(wave, resp, occ, idx, grad, local):
    t, hu = np_tables()
    f32, bf = jnp.float32, jnp.bfloat16
    consts = [jnp.asarray(v, bf) for v in (t, np.concatenate(y_tables(t)), dense_tables(hu), np.concatenate([hu, hu], axis=1))]
    consts += [jnp.asarray(v, f32) for v in inverse_tables(hu)]
    consts.append(jnp.asarray(x_table(hu), bf))
    vm, hbm = pl.BlockSpec(memory_space=pltpu.VMEM), pl.BlockSpec(memory_space=pl.ANY)
    dma = pltpu.SemaphoreType.DMA
    buf = lambda *dims: pltpu.VMEM(dims, f32)
    return pl.pallas_call(
        kernel,
        out_shape=jax.ShapeDtypeStruct((6, 576), f32),
        in_specs=[hbm] * (6 + len(consts)),
        out_specs=vm,
        scratch_shapes=[
            *(pltpu.VMEM(v.shape, v.dtype) for v in consts),
            pltpu.SMEM((256,), jnp.int32), pltpu.SMEM((1,), jnp.int32),
            pltpu.VMEM((NB, 2, 2, 96, BL), bf),
            buf(2, 96 * STEP, 128), buf(2, 96 * STEP, 128), buf(9, 864, 128), buf(9, 432, 128), buf(9, 4, 4, 3, 8, 128),
            buf(9, 3, 3, 4, 8, 128), buf(9, 3, 4, 8, 128), buf(9, 3, 3, 8, 128), buf(96, 384), buf(3, 96, 128),
            buf(8, 36, 128), buf(7, 36, 128), buf(8, 36, 128), buf(7, 36, 128), buf(256, 128), buf(256, 128),
            buf(16, 16, 128), buf(16, 16, 128), buf(2, 16, 128), buf(2, 6, 9984), buf(2, 96, 128), buf(96, 128),
            dma((NB,)), dma((7,)), dma((1,)), dma((2,)), dma((1,)), dma((3,)), dma((1,)), dma((3,)), dma((1,)), dma((3,)),
            *(dma((1,)) for _ in range(6)), dma((2,)), dma((2,)), dma((1,)), dma((1,)),
        ],
        compiler_params=pltpu.CompilerParams(collective_id=0, has_side_effects=True, vmem_limit_bytes=60 * 1024 * 1024),
        name="response",
    )(occ, idx, wave, resp, grad, local, *consts)


def shards(wave_coeff, response_coeff, band_index, occupation, local_kernel, gradient_kernel):
    return run(wave_coeff, response_coeff, occupation, band_index, gradient_kernel, local_kernel)


def solution(mesh):
    return jax.shard_map(
        shards,
        mesh=mesh,
        in_specs=(
            P(("pool", "slab"), None, None, None),
            P(("pool", "slab"), None, None, None),
            P(("pool", "slab")),
            P(),
            P("slab", None),
            P("slab", None),
        ),
        out_specs=P("slab", "pool"),
        check_vma=False,
    )
```

```python
import math

import numpy as np
import jax
import jax.numpy as jnp
from jax import lax
from jax.experimental import pallas as pl
from jax.experimental.pallas import tpu as pltpu
from jax.sharding import PartitionSpec as P

MESH = pl.DeviceIdType.MESH
full_turn = 2.0 * math.pi
N = 96
BL = 1536
NB = 9216 // BL
STEP = 97


def np_tables():
    k = np.arange(N)
    ang = (np.outer(k, k) % N) * (2 * np.pi / N)
    c, s = np.cos(ang) / np.sqrt(N), np.sin(ang) / np.sqrt(N)
    t = np.block([[c, -s], [s, c]])
    return t, np.cos(ang) + np.sin(ang)


def y_tables(t):
    outs = []
    for skip in (0, 32):
        w = np.zeros((256, 256))
        for s in range(2):
            for r in range(2):
                w[128 * s + skip:128 * s + skip + 96, 128 * r:128 * r + 96] = t[96 * r:96 * r + 96, 96 * s:96 * s + 96].T
        outs.append(w)
    return outs


def dense_tables(hu):
    outs = []
    for j in range(3):
        w = np.zeros((256, 128))
        for l in range(128):
            q, ky = divmod(128 * j + l, 96)
            w[(q - j) * 128:(q - j) * 128 + 96, l] = hu[ky]
        outs.append(np.concatenate([w, w], axis=0))
    return np.stack(outs)


def inverse_tables(hu):
    hye = np.zeros((128, 128))
    hye[:N] = hu[:, (np.arange(128) - 16) % N] / N
    return [hu / math.sqrt(N), hye]


def x_table(hu):
    w = np.zeros((16, 16, 32, 8))
    for p in range(16):
        for i in range(10):
            w[p, i, :, :3] = (hu[(6 * p - 2 + i) % N] / N).reshape(32, 3)
    w = w.reshape(256, 256)
    hi = w.astype(jnp.bfloat16).astype(np.float64)
    return np.concatenate([hi, hi, w - hi], axis=1)


def halves(v):
    hi = v.astype(jnp.bfloat16)
    return hi, (v - hi.astype(jnp.float32)).astype(jnp.bfloat16)


def close(a, b):
    (ah, al), (bh, bl) = halves(a), halves(b)
    return jnp.dot(jnp.concatenate([ah, ah, al], axis=1), jnp.concatenate([bh, bl, bh], axis=0), preferred_element_type=jnp.float32)


def kernel(occupation, numbers, wave, resp, grad, local, *refs):
    tables, out, held, refs = refs[:7], refs[7], refs[8:15], refs[15:]
    (occ, idx, cc, rs, bw, br, d, pbuf, s, f1, t2, f3, zbuf, rbuf, zp, zpr, zv, zvr, q, a, xo, b, gr, flat, gl, pot,
     csem, tsem, gsem, osem, p_snd, p_rcv, s1, r1, s3, r3, sp, rp, sv, rv, sa, ra, sb, rb, sg, rg) = refs
    t_ref, wy, yd, hx, hz, hye, hxe = held
    f32, bf = jnp.float32, jnp.bfloat16
    pool, slab = lax.axis_index("pool"), lax.axis_index("slab")
    y, x = pool // 4, pool % 4
    zc, core = slab // 2, slab % 2
    other = 1 - core

    def load(k, blk):
        return pltpu.make_async_copy((wave, resp)[k].at[0, :, :, pl.ds(blk * BL, BL)], cc.at[blk, k], csem.at[blk])

    early = [pltpu.make_async_copy(tables[n], held[n], tsem.at[n]) for n in range(2)]
    late = [pltpu.make_async_copy(tables[n], held[n], tsem.at[n]) for n in range(2, 7)]
    for cp in early:
        cp.start()
    for blk in range(NB):
        for k in range(2):
            load(k, blk).start()
    for cp in late:
        cp.start()
    weights = [pltpu.make_async_copy(occupation, occ, osem.at[0]), pltpu.make_async_copy(numbers, idx, osem.at[1])]
    for cp in weights:
        cp.start()
    for k, src in enumerate((grad, local)):
        for lo, to, size in ((0, 384, 9216), (9216 - 384, 0, 384), (0, 9600, 384)):
            pltpu.make_async_copy(src.at[:, pl.ds(lo, size)], flat.at[k, :, pl.ds(to, size)], gsem.at[0]).start()

    def drain(ref, sem):
        pltpu.make_async_copy(ref, ref, sem).wait()


    def dev(p, sl):
        return {"pool": p, "slab": sl}

    def plane(k):
        dc, dp = k // 16, k % 16
        c2 = (core + dc) % 2
        p2 = (pool + dp) % 16
        return c2, p2, dev(p2, zc * 2 + c2)

    barrier = pltpu.get_barrier_semaphore()

    def hail(who):
        pl.semaphore_signal(barrier, inc=1, device_id=who, device_id_type=MESH)

    for k in range(1, 32):
        hail(plane(k)[2])
    for dz in range(1, 8):
        hail(dev(pool, (slab + 2 * dz) % 16))
    hail(dev(pool, (slab + 15 + 2 * core) % 16))
    for r in range(12, 16):
        hail(dev(r, (slab + (1 if r < 14 else 15)) % 16))

    def send(src, dst, ssem, rsem, who):
        cp = pltpu.make_async_remote_copy(src_ref=src, dst_ref=dst, send_sem=ssem, recv_sem=rsem, device_id=who, device_id_type=MESH)
        cp.start()
        return cp

    for ref in (q, a, b):
        ref[...] = jnp.zeros_like(ref)
    for cp in early:
        cp.wait()

    def first_phase(blk, carry):
        drain(cc.at[blk], csem.at[blk])
        t = t_ref[...]
        for k, dst in enumerate((bw, br)):
            c = jnp.concatenate([cc[blk, k, 0], cc[blk, k, 1]], axis=0)
            zb = jnp.dot(t, c, preferred_element_type=f32).astype(bf)
            groups = BL // 384
            for row, (start, lo) in enumerate(((0, 0), (96, 0), (192, 0), (256, 256))):
                lhs = jnp.concatenate([
                    jnp.concatenate([zb[96 * r:96 * r + 96, 384 * n + start:384 * n + start + 128] for r in range(2)], axis=1)
                    for n in range(groups)], axis=0)
                res = jnp.dot(lhs, wy[lo:lo + 256], preferred_element_type=f32)
                for n in range(groups):
                    base = (blk * (BL // 96) + 4 * n + row) * STEP
                    for r in range(2):
                        dst[r, pl.ds(base, 96), :] = res[96 * n:96 * n + 96, 128 * r:128 * r + 128]
        return carry

    def to_space(chunk, planes):
        t = t_ref[...]
        weight = occ[idx[0]].astype(f32) * (1.0 / 256.0)
        for lo in (0, 4):
            spaces = []
            for src in (bw, br):
                parts = []
                for k, i in planes[lo:lo + 4]:
                    parts.append(jnp.concatenate([src[r, pl.ds(32 * chunk + 8 * k + i, 96, stride=STEP), :].astype(bf) for r in range(2)], axis=0))
                spaces.append(jnp.dot(t, jnp.concatenate(parts, axis=1), preferred_element_type=f32))
            v, w = spaces
            pair = halves((v[:96] * w[:96] + v[96:] * w[96:]) * weight)
            for n, (k, i) in enumerate(planes[lo:lo + 4]):
                for h in range(2):
                    rs[h, k, pl.ds(i * 96, 96), :] = pair[h][:, 128 * n:128 * n + 128]

    def to_waves(u, j):
        lhs = jnp.concatenate([rs[h, j + n] for h in range(2) for n in range(2)], axis=1)
        col = jnp.dot(lhs, yd[j], preferred_element_type=f32)
        col = jnp.concatenate([col[96 * i:96 * i + 96] for i in range(8)], axis=1)
        gx = jnp.dot(hx[...], jnp.concatenate(halves(col), axis=0), preferred_element_type=f32)
        for i in range(8):
            d[u, pl.ds(i, 96, stride=9), :] = gx[:, 128 * i:128 * i + 128]

    def unit(u):
        c, j = divmod(u, 3)
        with jax.named_scope(f"unit{u}"):
            if j == 0:
                to_space(c, [(k, i) for i in range(4) for k in range(2)])
                to_space(c, [(k, i) for i in range(4, 8) for k in range(2)])
            else:
                to_space(c, [(j + 1, i) for i in range(8)])
            to_waves(u, j)


    def order(u, m, along):
        ax = (3 * u + m + along) % 2
        return (x, y)[ax], ax

    def at(ax, pos):
        return dev(y * 4 + pos, slab) if ax == 0 else dev(pos * 4 + x, slab)

    def units(c):
        return range(3 * c, 3 * c + 3)

    def start_pair(u):
        send(d.at[u, pl.ds(pl.multiple_of(other * 432, 432), 432)], pbuf.at[u], p_snd.at[0], p_rcv.at[u], dev(pool, zc * 2 + other))

    def start_a(u):
        with jax.named_scope(f"a{u}"):
            drain(pbuf.at[u], p_rcv.at[u])
            for n in range(48):
                s[u, n // 12, n // 3 % 4, n % 3] = d[u, pl.ds(core * 432 + 9 * n, 8), :] + pbuf[u, pl.ds(9 * n, 8), :]
            for m in range(3):
                pos, ax = order(u, m, 0)
                for k in (2, 1, 3):
                    to = (pos + k) % 4
                    src = s.at[u, :, to, m] if ax == 0 else s.at[u, to, :, m]
                    send(src, f1.at[u, m, k - 1], s1.at[0], r1.at[u], at(ax, to))

    def start_b(u):
        with jax.named_scope(f"b{u}"):
            drain(f1.at[u], r1.at[u])
            for m in range(3):
                pos, ax = order(u, m, 0)
                part = s[u, :, pos, m] if ax == 0 else s[u, pos, :, m]
                for k in (1, 3, 2):
                    part = part + f1[u, m, k - 1]
                t2[u, m] = part
                pos, ax = order(u, m, 1)
                for k in (2, 1, 3):
                    to = (pos + k) % 4
                    send(t2.at[u, m, to], f3.at[u, m, k - 1], s3.at[0], r3.at[u // 3], at(ax, to))

    lane = lax.broadcasted_iota(jnp.int32, (8, 128), 1)

    def finish(c):
        parts = {}
        drain(f3.at[pl.ds(3 * c, 3)], r3.at[c])
        for u in units(c):
            for m in range(3):
                part = t2[u, m, order(u, m, 1)[0]]
                for k in (1, 3, 2):
                    part = part + f3[u, m, k - 1]
                parts[u - 3 * c, m] = part
        for m in range(3):
            v = jnp.concatenate([parts[j, m] for j in range(3)], axis=1)
            for k in range(4):
                w = v if k == 0 else pltpu.roll(v, 384 - 96 * k, 1)
                zbuf[32 * c + 8 * k:32 * c + 8 * k + 8, 128 * m:128 * m + 128] = jnp.where(lane < 96, w[:, :128], 0.0)
        rows = jnp.concatenate([zbuf[32 * c:32 * c + 32, 128 * m:128 * m + 128] for m in range(3)], axis=0)
        both = close(rows, hye[...])
        for m in range(3):
            rbuf[m, 32 * c:32 * c + 32, :] = both[32 * m:32 * m + 32]
        for zd in ((0, 1), (2, 3, 4), (5, 6, 7))[c]:
            for m in range(3):
                zp[zd, 12 * m:12 * m + 12, :] = rbuf[m, 12 * zd:12 * zd + 12, :]
            slot = (zd - zc + 15) % 8
            cp = pltpu.make_async_remote_copy(src_ref=zp.at[zd], dst_ref=zpr.at[slot], send_sem=sp.at[0], recv_sem=rp.at[0], device_id=dev(pool, 2 * zd + core), device_id_type=MESH)
            pl.when(zc != zd)(cp.start)

    with jax.named_scope("first_phase"):
        lax.fori_loop(0, NB, first_phase, 0)
    for cp in late + weights:
        cp.wait()
    unit(0)
    with jax.named_scope("barrier"):
        pl.semaphore_wait(barrier, 39 + 16 * (pool // 12))
    start_pair(0)
    for u in range(1, 9):
        unit(u)
        start_pair(u)
        start_a(u - 1)
        if u >= 5:
            start_b(u - 5)
    start_a(8)
    start_b(4)
    with jax.named_scope("finish0"):
        finish(0)
    for u in (5, 6, 7, 8):
        start_b(u)
    with jax.named_scope("finish1"):
        finish(1)
    with jax.named_scope("finish2"):
        finish(2)

    with jax.named_scope("solve"):
        zk = zbuf[...]
        vh = close(hz[...], zk)
        kz = lax.broadcasted_iota(jnp.int32, (96, 128), 0)
        ky = lax.broadcasted_iota(jnp.int32, (96, 128), 1)
        qz = jnp.where(2 * kz >= N, kz - N, kz)
        qy = jnp.where(2 * ky >= N, ky - N, ky)
        zy = qz * qz + qy * qy
        scaled = []
        for m in range(3):
            kx = jnp.full((96, 128), 1, jnp.int32) * (3 * (core * 16 + pool) + m)
            qx = jnp.where(2 * kx >= N, kx - N, kx)
            squared = (zy + qx * qx).astype(f32) * ((full_turn / N) ** 2)
            screen = jnp.where(squared > 0, full_turn / jnp.where(squared > 0, squared, 1.0), 0.0)
            scaled.append(vh[:, 128 * m:128 * m + 128] * screen)
        vz = close(hz[...], jnp.concatenate(scaled, axis=1))
        both = close(jnp.concatenate([vz[:, 128 * m:128 * m + 128] for m in range(3)], axis=0), hye[...])
        for m in range(3):
            for zd in range(8):
                zv[zd, 12 * m:12 * m + 12, :] = both[96 * m + 12 * zd:96 * m + 12 * zd + 12]

    with jax.named_scope("zstage"):
        def col(k):
            return dev(pool, ((zc + k) % 8) * 2 + core)
        for k in (4, 3, 5, 2, 6, 1, 7):
            send(zv.at[(zc + k) % 8], zvr.at[k - 1], sv.at[0], rv.at[0], col(k))
        drain(flat, gsem.at[0])
        odd = pool % 2
        wide = lax.broadcasted_iota(jnp.int32, (6, 128), 1)
        for k in range(2):
            v = flat[k, :, pl.ds(pl.multiple_of(576 * pool - 64 * odd, 128), 1408)]
            v = jnp.where(odd == 1, pltpu.roll(v, 1408 - 64, 1), v)
            wins = [v[:, 176 + 96 * w:304 + 96 * w] for w in range(-1, 11)]
            for w in range(10):
                gl[k, pl.ds(w, 6, stride=16), :] = jnp.where(wide < 16, wins[w + 2], jnp.where(wide >= 112, wins[w], wins[w + 1]))
        send(gl.at[0, pl.ds(80, 16)], gr.at[0], sg.at[0], rg.at[0], dev(pool, (slab + 1) % 16))
        send(gl.at[0, pl.ds(0, 16)], gr.at[1], sg.at[0], rg.at[0], dev(pool, (slab + 15) % 16))

    me = core * 16 + pool
    mine = pl.ds(pl.multiple_of(me * 8, 8), 3)

    def deal(rows):
        for dc in range(2):
            c2 = (core + dc) % 2
            for r in rows:
                src = q.at[pl.ds(pl.multiple_of((c2 * 16 + r) * 8, 8), 3)]
                cp = pltpu.make_async_remote_copy(src_ref=src, dst_ref=a.at[mine], send_sem=sa.at[0], recv_sem=ra.at[0], device_id=dev(r, zc * 2 + c2), device_id_type=MESH)
                if dc:
                    cp.start()
                else:
                    pl.when(pool != r)(cp.start)

    with jax.named_scope("rows_rho"):
        drain(zpr, rp.at[0])
        f = zp[zc]
        for k in range(7):
            f = f + zpr[k]
        for c2 in range(2):
            for m in range(3):
                base = c2 * 128 + m
                rho6 = f[12 * m + 6 * c2:12 * m + 6 * c2 + 6]
                q[pl.ds(base, 6, stride=8), :] = rho6
                q[pl.ds(base + 96, 2, stride=8), :] = rho6[:2]
                q[pl.ds(base + 112, 2, stride=8), :] = rho6[4:]
        deal((0, 1, 2, 3, 4, 5, 12, 13, 14, 15))
    with jax.named_scope("rows_v"):
        drain(zvr, rv.at[0])
        f = zv[zc]
        for k in range(7):
            f = f + zvr[k]
        for c2 in range(2):
            for m in range(3):
                q[pl.ds(c2 * 128 + m + 48, 6, stride=8), :] = f[12 * m + 6 * c2:12 * m + 6 * c2 + 6]
        deal(range(6, 12))
    with jax.named_scope("rows_out"):
        a[mine, :] = q[pl.ds(pl.multiple_of((core * 16 + pool) * 8, 8), 3), :]
        drain(a.at[pl.ds(0, 93)], ra.at[0])
    with jax.named_scope("rows_back"):
        hi, lo = halves(a[...])
        xo[...] = jnp.dot(hxe[...], jnp.concatenate([hi, lo, hi], axis=0), preferred_element_type=f32).reshape(16, 16, 128)
        edge = pool // 12
        aim = (slab + 16 + edge * (2 * (pool // 14) - 1)) % 16
        for k in range(1, 16):
            p2 = (pool + k) % 16
            send(xo.at[p2, pl.ds(0, 10)], b.at[pool, pl.ds(0, 10)], sb.at[0], rb.at[0], dev(p2, aim))

        def across():
            return pltpu.make_async_remote_copy(src_ref=xo.at[pool, pl.ds(0, 10)], dst_ref=b.at[pool, pl.ds(0, 10)], send_sem=sb.at[1], recv_sem=rb.at[1], device_id=dev(pool, aim), device_id_type=MESH)

        @pl.when(edge == 0)
        def _():
            b[pool] = xo[pool]

        @pl.when(edge == 1)
        def _():
            across().start()
            across().wait()
        drain(gr, rg.at[0])
        drain(a.at[pl.ds(0, 150)], rb.at[0])

    with jax.named_scope("final"):
        def up(v, ax):
            return pltpu.roll(v, v.shape[ax] - 1, ax)

        def down(v, ax):
            return pltpu.roll(v, 1, ax)
        g = [gl[0, pl.ds(16 * n, 16), :] for n in range(6)]
        rhos = [b[n] for n in (14, 15, 0, 1, 2, 3, 4, 5, 12, 13)]
        flux = []
        for n in range(8):
            coef = gr[0] if n == 0 else gr[1] if n == 7 else g[n - 1]
            flux.append(coef * ((rhos[n + 2] - rhos[n]) * 0.5))
        for n in range(6):
            rho, coef = rhos[n + 2], g[n]
            div = (flux[n + 2] - flux[n]) * 0.5
            for ax in (0, 1):
                slope = coef * ((up(rho, ax) - down(rho, ax)) * 0.5)
                div = div + (up(slope, ax) - down(slope, ax)) * 0.5
            pot[pl.ds(16 * n, 16), :] = b[6 + n] + gl[1, pl.ds(16 * n, 16), :] * rho - div
        row640 = lax.broadcasted_iota(jnp.int32, (6, 640), 1)
        whole = jnp.zeros((6, 640), f32)
        for w in range(6):
            piece = jnp.concatenate([pot[pl.ds(w + 2, 6, stride=16), :], jnp.zeros((6, 512), f32)], axis=1)
            piece = pltpu.roll(piece, (96 * w - 16) % 640, 1)
            whole = jnp.where((row640 >= 96 * w) & (row640 < 96 * w + 96), piece, whole)
        out[...] = whole[:, :576]

    with jax.named_scope("sent"):
        for ref, sem in ((pbuf, p_snd), (f1, s1), (f3, s3), (zpr, sp), (zvr, sv), (gr, sg), (a.at[pl.ds(0, 93)], sa), (a.at[pl.ds(0, 150)], sb)):
            drain(ref, sem.at[0])


def run(wave, resp, occ, idx, grad, local):
    t, hu = np_tables()
    f32, bf = jnp.float32, jnp.bfloat16
    consts = [jnp.asarray(v, bf) for v in (t, np.concatenate(y_tables(t)), dense_tables(hu), np.concatenate([hu, hu], axis=1))]
    consts += [jnp.asarray(v, f32) for v in inverse_tables(hu)]
    consts.append(jnp.asarray(x_table(hu), bf))
    vm, hbm = pl.BlockSpec(memory_space=pltpu.VMEM), pl.BlockSpec(memory_space=pltpu.HBM)
    dma = pltpu.SemaphoreType.DMA
    buf = lambda *dims: pltpu.VMEM(dims, f32)
    return pl.pallas_call(
        kernel,
        out_shape=pltpu.VMEM((6, 576), f32),
        in_specs=[hbm] * (6 + len(consts)),
        out_specs=vm,
        scratch_shapes=[
            *(pltpu.VMEM(v.shape, v.dtype) for v in consts),
            pltpu.SMEM((256,), jnp.int32), pltpu.SMEM((1,), jnp.int32),
            pltpu.VMEM((NB, 2, 2, 96, BL), bf), pltpu.VMEM((2, 4, 768, 128), bf),
            buf(2, 96 * STEP, 128), buf(2, 96 * STEP, 128), buf(9, 864, 128), buf(9, 432, 128), buf(9, 4, 4, 3, 8, 128),
            buf(9, 3, 3, 4, 8, 128), buf(9, 3, 4, 8, 128), buf(9, 3, 3, 8, 128), buf(96, 384), buf(3, 96, 128),
            buf(8, 36, 128), buf(7, 36, 128), buf(8, 36, 128), buf(7, 36, 128), buf(256, 128), buf(256, 128),
            buf(16, 16, 128), buf(16, 16, 128), buf(2, 16, 128), buf(2, 6, 9984), buf(2, 96, 128), buf(96, 128),
            dma((NB,)), dma((7,)), dma((1,)), dma((2,)), dma((1,)), dma((9,)), dma((1,)), dma((9,)), dma((1,)), dma((3,)),
            *(dma((1,)) for _ in range(6)), dma((2,)), dma((2,)), dma((1,)), dma((1,)),
        ],
        compiler_params=pltpu.CompilerParams(collective_id=0, has_side_effects=True, vmem_limit_bytes=60 * 1024 * 1024),
        name="response",
    )(occ, idx, wave, resp, grad, local, *consts)


def shards(wave_coeff, response_coeff, band_index, occupation, local_kernel, gradient_kernel):
    return run(wave_coeff, response_coeff, occupation, band_index, gradient_kernel, local_kernel)


def solution(mesh):
    return jax.shard_map(
        shards,
        mesh=mesh,
        in_specs=(
            P(("pool", "slab"), None, None, None),
            P(("pool", "slab"), None, None, None),
            P(("pool", "slab")),
            P(),
            P("slab", None),
            P("slab", None),
        ),
        out_specs=P("slab", "pool"),
        check_vma=False,
    )
```

```python
import math

import numpy as np
import jax
import jax.numpy as jnp
from jax import lax
from jax.experimental import pallas as pl
from jax.experimental.pallas import tpu as pltpu
from jax.sharding import PartitionSpec as P

MESH = pl.DeviceIdType.MESH
full_turn = 2.0 * math.pi
N = 96
BL = 1536
NB = 9216 // BL
STEP = 97


def np_tables():
    k = np.arange(N)
    ang = (np.outer(k, k) % N) * (2 * np.pi / N)
    c, s = np.cos(ang) / np.sqrt(N), np.sin(ang) / np.sqrt(N)
    t = np.block([[c, -s], [s, c]])
    return t, np.cos(ang) + np.sin(ang)


def y_tables(t):
    outs = []
    for skip in (0, 32):
        w = np.zeros((256, 256))
        for s in range(2):
            for r in range(2):
                w[128 * s + skip:128 * s + skip + 96, 128 * r:128 * r + 96] = t[96 * r:96 * r + 96, 96 * s:96 * s + 96].T
        outs.append(w)
    return outs


def dense_tables(hu):
    outs = []
    for j in range(3):
        w = np.zeros((256, 128))
        for l in range(128):
            q, ky = divmod(128 * j + l, 96)
            w[(q - j) * 128:(q - j) * 128 + 96, l] = hu[ky]
        outs.append(w)
    return np.stack(outs)


def inverse_tables(hu):
    hye = np.zeros((128, 128))
    hye[:N] = hu[:, (np.arange(128) - 16) % N] / N
    return [hu / math.sqrt(N), hye]


def x_table(hu):
    w = np.zeros((16, 16, 32, 8))
    for p in range(16):
        for i in range(10):
            w[p, i, :, :3] = (hu[(6 * p - 2 + i) % N] / N).reshape(32, 3)
    w = w.reshape(256, 256)
    hi = w.astype(jnp.bfloat16).astype(np.float64)
    return np.concatenate([hi, hi, w - hi], axis=1)


def halves(v):
    hi = v.astype(jnp.bfloat16)
    return hi, (v - hi.astype(jnp.float32)).astype(jnp.bfloat16)


def close(a, b):
    (ah, al), (bh, bl) = halves(a), halves(b)
    return jnp.dot(jnp.concatenate([ah, ah, al], axis=1), jnp.concatenate([bh, bl, bh], axis=0), preferred_element_type=jnp.float32)


def kernel(occupation, numbers, wave, resp, grad, local, *refs):
    tables, out, held, refs = refs[:7], refs[7], refs[8:15], refs[15:]
    (occ, idx, cc, rs, bw, br, d, pbuf, s, f1, t2, f3, zbuf, rbuf, zp, zpr, zv, zvr, q, a, xo, b, gr, flat, gl, pot,
     csem, tsem, gsem, osem, p_snd, p_rcv, s1, r1, s3, r3, sp, rp, sv, rv, sa, ra, sb, rb, sg, rg) = refs
    t_ref, wy, yd, hx, hz, hye, hxe = held
    f32, bf = jnp.float32, jnp.bfloat16
    pool, slab = lax.axis_index("pool"), lax.axis_index("slab")
    y, x = pool // 4, pool % 4
    zc, core = slab // 2, slab % 2
    other = 1 - core

    def load(k, blk):
        return pltpu.make_async_copy((wave, resp)[k].at[0, :, :, pl.ds(blk * BL, BL)], cc.at[blk, k], csem.at[blk])

    early = [pltpu.make_async_copy(tables[n], held[n], tsem.at[n]) for n in range(2)]
    late = [pltpu.make_async_copy(tables[n], held[n], tsem.at[n]) for n in range(2, 7)]
    for cp in early:
        cp.start()
    for blk in range(NB):
        for k in range(2):
            load(k, blk).start()
    for cp in late:
        cp.start()
    weights = [pltpu.make_async_copy(occupation, occ, osem.at[0]), pltpu.make_async_copy(numbers, idx, osem.at[1])]
    for cp in weights:
        cp.start()
    for k, src in enumerate((grad, local)):
        for lo, to, size in ((0, 384, 9216), (9216 - 384, 0, 384), (0, 9600, 384)):
            pltpu.make_async_copy(src.at[:, pl.ds(lo, size)], flat.at[k, :, pl.ds(to, size)], gsem.at[0]).start()

    def drain(ref, sem):
        pltpu.make_async_copy(ref, ref, sem).wait()


    def dev(p, sl):
        return {"pool": p, "slab": sl}

    def plane(k):
        dc, dp = k // 16, k % 16
        c2 = (core + dc) % 2
        p2 = (pool + dp) % 16
        return c2, p2, dev(p2, zc * 2 + c2)

    barrier = pltpu.get_barrier_semaphore()

    def hail(who):
        pl.semaphore_signal(barrier, inc=1, device_id=who, device_id_type=MESH)

    for k in range(1, 32):
        hail(plane(k)[2])
    for dz in range(1, 8):
        hail(dev(pool, (slab + 2 * dz) % 16))
    hail(dev(pool, (slab + 15 + 2 * core) % 16))
    for r in range(12, 16):
        hail(dev(r, (slab + (1 if r < 14 else 15)) % 16))

    def send(src, dst, ssem, rsem, who):
        cp = pltpu.make_async_remote_copy(src_ref=src, dst_ref=dst, send_sem=ssem, recv_sem=rsem, device_id=who, device_id_type=MESH)
        cp.start()
        return cp

    for ref in (q, a, b):
        ref[...] = jnp.zeros_like(ref)
    for cp in early:
        cp.wait()

    def first_phase(blk, carry):
        drain(cc.at[blk], csem.at[blk])
        t = t_ref[...]
        for k, dst in enumerate((bw, br)):
            c = jnp.concatenate([cc[blk, k, 0], cc[blk, k, 1]], axis=0)
            zb = jnp.dot(t, c, preferred_element_type=f32).astype(bf)
            groups = BL // 384
            for row, (start, lo) in enumerate(((0, 0), (96, 0), (192, 0), (256, 256))):
                lhs = jnp.concatenate([
                    jnp.concatenate([zb[96 * r:96 * r + 96, 384 * n + start:384 * n + start + 128] for r in range(2)], axis=1)
                    for n in range(groups)], axis=0)
                res = jnp.dot(lhs, wy[lo:lo + 256], preferred_element_type=f32)
                for n in range(groups):
                    base = (blk * (BL // 96) + 4 * n + row) * STEP
                    for r in range(2):
                        dst[r, pl.ds(base, 96), :] = res[96 * n:96 * n + 96, 128 * r:128 * r + 128]
        return carry

    def to_space(chunk, planes):
        t = t_ref[...]
        weight = occ[idx[0]].astype(f32) * (1.0 / 256.0)
        for lo in (0, 4):
            spaces = []
            for src in (bw, br):
                parts = []
                for k, i in planes[lo:lo + 4]:
                    parts.append(jnp.concatenate([src[r, pl.ds(32 * chunk + 8 * k + i, 96, stride=STEP), :].astype(bf) for r in range(2)], axis=0))
                spaces.append(jnp.dot(t, jnp.concatenate(parts, axis=1), preferred_element_type=f32))
            v, w = spaces
            rho = ((v[:96] * w[:96] + v[96:] * w[96:]) * weight).astype(bf)
            for n, (k, i) in enumerate(planes[lo:lo + 4]):
                rs[k, pl.ds(i * 96, 96), :] = rho[:, 128 * n:128 * n + 128]

    def to_waves(u, j):
        lhs = jnp.concatenate([rs[j], rs[j + 1]], axis=1)
        col = jnp.dot(lhs, yd[j], preferred_element_type=f32)
        col = jnp.concatenate([col[96 * i:96 * i + 96] for i in range(8)], axis=1)
        gx = jnp.dot(hx[...], jnp.concatenate(halves(col), axis=0), preferred_element_type=f32)
        for i in range(8):
            d[u, pl.ds(i, 96, stride=9), :] = gx[:, 128 * i:128 * i + 128]

    def unit(u):
        c, j = divmod(u, 3)
        with jax.named_scope(f"unit{u}"):
            if j == 0:
                to_space(c, [(k, i) for i in range(4) for k in range(2)])
                to_space(c, [(k, i) for i in range(4, 8) for k in range(2)])
            else:
                to_space(c, [(j + 1, i) for i in range(8)])
            to_waves(u, j)


    def order(u, m, along):
        ax = (3 * u + m + along) % 2
        return (x, y)[ax], ax

    def at(ax, pos):
        return dev(y * 4 + pos, slab) if ax == 0 else dev(pos * 4 + x, slab)

    def units(c):
        return range(3 * c, 3 * c + 3)

    def start_pair(u):
        send(d.at[u, pl.ds(pl.multiple_of(other * 432, 432), 432)], pbuf.at[u], p_snd.at[0], p_rcv.at[u], dev(pool, zc * 2 + other))

    def start_a(u):
        with jax.named_scope(f"a{u}"):
            drain(pbuf.at[u], p_rcv.at[u])
            for n in range(48):
                s[u, n // 12, n // 3 % 4, n % 3] = d[u, pl.ds(core * 432 + 9 * n, 8), :] + pbuf[u, pl.ds(9 * n, 8), :]
            for m in range(3):
                pos, ax = order(u, m, 0)
                for k in (2, 1, 3):
                    to = (pos + k) % 4
                    src = s.at[u, :, to, m] if ax == 0 else s.at[u, to, :, m]
                    send(src, f1.at[u, m, k - 1], s1.at[0], r1.at[u], at(ax, to))

    def start_b(u):
        with jax.named_scope(f"b{u}"):
            drain(f1.at[u], r1.at[u])
            for m in range(3):
                pos, ax = order(u, m, 0)
                part = s[u, :, pos, m] if ax == 0 else s[u, pos, :, m]
                for k in (1, 3, 2):
                    part = part + f1[u, m, k - 1]
                t2[u, m] = part
                pos, ax = order(u, m, 1)
                for k in (2, 1, 3):
                    to = (pos + k) % 4
                    send(t2.at[u, m, to], f3.at[u, m, k - 1], s3.at[0], r3.at[u // 3], at(ax, to))

    lane = lax.broadcasted_iota(jnp.int32, (8, 128), 1)

    def finish(c):
        parts = {}
        drain(f3.at[pl.ds(3 * c, 3)], r3.at[c])
        for u in units(c):
            for m in range(3):
                part = t2[u, m, order(u, m, 1)[0]]
                for k in (1, 3, 2):
                    part = part + f3[u, m, k - 1]
                parts[u - 3 * c, m] = part
        for m in range(3):
            v = jnp.concatenate([parts[j, m] for j in range(3)], axis=1)
            for k in range(4):
                w = v if k == 0 else pltpu.roll(v, 384 - 96 * k, 1)
                zbuf[32 * c + 8 * k:32 * c + 8 * k + 8, 128 * m:128 * m + 128] = jnp.where(lane < 96, w[:, :128], 0.0)
        rows = jnp.concatenate([zbuf[32 * c:32 * c + 32, 128 * m:128 * m + 128] for m in range(3)], axis=0)
        both = close(rows, hye[...])
        for m in range(3):
            rbuf[m, 32 * c:32 * c + 32, :] = both[32 * m:32 * m + 32]
        for zd in ((0, 1), (2, 3, 4), (5, 6, 7))[c]:
            for m in range(3):
                zp[zd, 12 * m:12 * m + 12, :] = rbuf[m, 12 * zd:12 * zd + 12, :]
            slot = (zd - zc + 15) % 8
            cp = pltpu.make_async_remote_copy(src_ref=zp.at[zd], dst_ref=zpr.at[slot], send_sem=sp.at[0], recv_sem=rp.at[0], device_id=dev(pool, 2 * zd + core), device_id_type=MESH)
            pl.when(zc != zd)(cp.start)

    with jax.named_scope("first_phase"):
        lax.fori_loop(0, NB, first_phase, 0)
    for cp in late + weights:
        cp.wait()
    unit(0)
    with jax.named_scope("barrier"):
        pl.semaphore_wait(barrier, 39 + 16 * (pool // 12))
    start_pair(0)
    for u in range(1, 9):
        unit(u)
        start_pair(u)
        if u >= 2:
            start_a(u - 2)
        if u >= 7:
            start_b(u - 7)
    start_a(7)
    start_b(2)
    start_a(8)
    for u in (3, 4, 5):
        start_b(u)
    with jax.named_scope("finish0"):
        finish(0)
    for u in (6, 7, 8):
        start_b(u)
    with jax.named_scope("finish1"):
        finish(1)
    with jax.named_scope("finish2"):
        finish(2)

    with jax.named_scope("solve"):
        zk = zbuf[...]
        vh = close(hz[...], zk)
        kz = lax.broadcasted_iota(jnp.int32, (96, 128), 0)
        ky = lax.broadcasted_iota(jnp.int32, (96, 128), 1)
        qz = jnp.where(2 * kz >= N, kz - N, kz)
        qy = jnp.where(2 * ky >= N, ky - N, ky)
        zy = qz * qz + qy * qy
        scaled = []
        for m in range(3):
            kx = jnp.full((96, 128), 1, jnp.int32) * (3 * (core * 16 + pool) + m)
            qx = jnp.where(2 * kx >= N, kx - N, kx)
            squared = (zy + qx * qx).astype(f32) * ((full_turn / N) ** 2)
            screen = jnp.where(squared > 0, full_turn / jnp.where(squared > 0, squared, 1.0), 0.0)
            scaled.append(vh[:, 128 * m:128 * m + 128] * screen)
        vz = close(hz[...], jnp.concatenate(scaled, axis=1))
        both = close(jnp.concatenate([vz[:, 128 * m:128 * m + 128] for m in range(3)], axis=0), hye[...])
        for m in range(3):
            for zd in range(8):
                zv[zd, 12 * m:12 * m + 12, :] = both[96 * m + 12 * zd:96 * m + 12 * zd + 12]

    with jax.named_scope("zstage"):
        def col(k):
            return dev(pool, ((zc + k) % 8) * 2 + core)
        for k in (4, 3, 5, 2, 6, 1, 7):
            send(zv.at[(zc + k) % 8], zvr.at[k - 1], sv.at[0], rv.at[0], col(k))
        drain(flat, gsem.at[0])
        odd = pool % 2
        wide = lax.broadcasted_iota(jnp.int32, (6, 128), 1)
        for k in range(2):
            v = flat[k, :, pl.ds(pl.multiple_of(576 * pool - 64 * odd, 128), 1408)]
            v = jnp.where(odd == 1, pltpu.roll(v, 1408 - 64, 1), v)
            wins = [v[:, 176 + 96 * w:304 + 96 * w] for w in range(-1, 11)]
            for w in range(10):
                gl[k, pl.ds(w, 6, stride=16), :] = jnp.where(wide < 16, wins[w + 2], jnp.where(wide >= 112, wins[w], wins[w + 1]))
        send(gl.at[0, pl.ds(80, 16)], gr.at[0], sg.at[0], rg.at[0], dev(pool, (slab + 1) % 16))
        send(gl.at[0, pl.ds(0, 16)], gr.at[1], sg.at[0], rg.at[0], dev(pool, (slab + 15) % 16))

    me = core * 16 + pool
    mine = pl.ds(pl.multiple_of(me * 8, 8), 3)

    def deal(rows):
        for dc in range(2):
            c2 = (core + dc) % 2
            for r in rows:
                src = q.at[pl.ds(pl.multiple_of((c2 * 16 + r) * 8, 8), 3)]
                cp = pltpu.make_async_remote_copy(src_ref=src, dst_ref=a.at[mine], send_sem=sa.at[0], recv_sem=ra.at[0], device_id=dev(r, zc * 2 + c2), device_id_type=MESH)
                if dc:
                    cp.start()
                else:
                    pl.when(pool != r)(cp.start)

    with jax.named_scope("rows_rho"):
        drain(zpr, rp.at[0])
        f = zp[zc]
        for k in range(7):
            f = f + zpr[k]
        for c2 in range(2):
            for m in range(3):
                base = c2 * 128 + m
                rho6 = f[12 * m + 6 * c2:12 * m + 6 * c2 + 6]
                q[pl.ds(base, 6, stride=8), :] = rho6
                q[pl.ds(base + 96, 2, stride=8), :] = rho6[:2]
                q[pl.ds(base + 112, 2, stride=8), :] = rho6[4:]
        deal((0, 1, 2, 3, 4, 5, 12, 13, 14, 15))
    with jax.named_scope("rows_v"):
        drain(zvr, rv.at[0])
        f = zv[zc]
        for k in range(7):
            f = f + zvr[k]
        for c2 in range(2):
            for m in range(3):
                q[pl.ds(c2 * 128 + m + 48, 6, stride=8), :] = f[12 * m + 6 * c2:12 * m + 6 * c2 + 6]
        deal(range(6, 12))
    with jax.named_scope("rows_out"):
        a[mine, :] = q[pl.ds(pl.multiple_of((core * 16 + pool) * 8, 8), 3), :]
        drain(a.at[pl.ds(0, 93)], ra.at[0])
    with jax.named_scope("rows_back"):
        hi, lo = halves(a[...])
        xo[...] = jnp.dot(hxe[...], jnp.concatenate([hi, lo, hi], axis=0), preferred_element_type=f32).reshape(16, 16, 128)
        edge = pool // 12
        aim = (slab + 16 + edge * (2 * (pool // 14) - 1)) % 16
        for k in range(1, 16):
            p2 = (pool + k) % 16
            send(xo.at[p2, pl.ds(0, 10)], b.at[pool, pl.ds(0, 10)], sb.at[0], rb.at[0], dev(p2, aim))

        def across():
            return pltpu.make_async_remote_copy(src_ref=xo.at[pool, pl.ds(0, 10)], dst_ref=b.at[pool, pl.ds(0, 10)], send_sem=sb.at[1], recv_sem=rb.at[1], device_id=dev(pool, aim), device_id_type=MESH)

        @pl.when(edge == 0)
        def _():
            b[pool] = xo[pool]

        @pl.when(edge == 1)
        def _():
            across().start()
            across().wait()
        drain(gr, rg.at[0])
        drain(a.at[pl.ds(0, 150)], rb.at[0])

    with jax.named_scope("final"):
        def up(v, ax):
            return pltpu.roll(v, v.shape[ax] - 1, ax)

        def down(v, ax):
            return pltpu.roll(v, 1, ax)
        g = [gl[0, pl.ds(16 * n, 16), :] for n in range(6)]
        rhos = [b[n] for n in (14, 15, 0, 1, 2, 3, 4, 5, 12, 13)]
        flux = []
        for n in range(8):
            coef = gr[0] if n == 0 else gr[1] if n == 7 else g[n - 1]
            flux.append(coef * ((rhos[n + 2] - rhos[n]) * 0.5))
        for n in range(6):
            rho, coef = rhos[n + 2], g[n]
            div = (flux[n + 2] - flux[n]) * 0.5
            for ax in (0, 1):
                slope = coef * ((up(rho, ax) - down(rho, ax)) * 0.5)
                div = div + (up(slope, ax) - down(slope, ax)) * 0.5
            pot[pl.ds(16 * n, 16), :] = b[6 + n] + gl[1, pl.ds(16 * n, 16), :] * rho - div
        row640 = lax.broadcasted_iota(jnp.int32, (6, 640), 1)
        whole = jnp.zeros((6, 640), f32)
        for w in range(6):
            piece = jnp.concatenate([pot[pl.ds(w + 2, 6, stride=16), :], jnp.zeros((6, 512), f32)], axis=1)
            piece = pltpu.roll(piece, (96 * w - 16) % 640, 1)
            whole = jnp.where((row640 >= 96 * w) & (row640 < 96 * w + 96), piece, whole)
        out[...] = whole[:, :576]

    with jax.named_scope("sent"):
        for ref, sem in ((pbuf, p_snd), (f1, s1), (f3, s3), (zpr, sp), (zvr, sv), (gr, sg), (a.at[pl.ds(0, 93)], sa), (a.at[pl.ds(0, 150)], sb)):
            drain(ref, sem.at[0])


def run(wave, resp, occ, idx, grad, local):
    t, hu = np_tables()
    f32, bf = jnp.float32, jnp.bfloat16
    consts = [jnp.asarray(v, bf) for v in (t, np.concatenate(y_tables(t)), dense_tables(hu), np.concatenate([hu, hu], axis=1))]
    consts += [jnp.asarray(v, f32) for v in inverse_tables(hu)]
    consts.append(jnp.asarray(x_table(hu), bf))
    vm, hbm = pl.BlockSpec(memory_space=pltpu.VMEM), pl.BlockSpec(memory_space=pltpu.HBM)
    dma = pltpu.SemaphoreType.DMA
    buf = lambda *dims: pltpu.VMEM(dims, f32)
    return pl.pallas_call(
        kernel,
        out_shape=pltpu.VMEM((6, 576), f32),
        in_specs=[hbm] * (6 + len(consts)),
        out_specs=vm,
        scratch_shapes=[
            *(pltpu.VMEM(v.shape, v.dtype) for v in consts),
            pltpu.SMEM((256,), jnp.int32), pltpu.SMEM((1,), jnp.int32),
            pltpu.VMEM((NB, 2, 2, 96, BL), bf), pltpu.VMEM((4, 768, 128), bf),
            buf(2, 96 * STEP, 128), buf(2, 96 * STEP, 128), buf(9, 864, 128), buf(9, 432, 128), buf(9, 4, 4, 3, 8, 128),
            buf(9, 3, 3, 4, 8, 128), buf(9, 3, 4, 8, 128), buf(9, 3, 3, 8, 128), buf(96, 384), buf(3, 96, 128),
            buf(8, 36, 128), buf(7, 36, 128), buf(8, 36, 128), buf(7, 36, 128), buf(256, 128), buf(256, 128),
            buf(16, 16, 128), buf(16, 16, 128), buf(2, 16, 128), buf(2, 6, 9984), buf(2, 96, 128), buf(96, 128),
            dma((NB,)), dma((7,)), dma((1,)), dma((2,)), dma((1,)), dma((9,)), dma((1,)), dma((9,)), dma((1,)), dma((3,)),
            *(dma((1,)) for _ in range(6)), dma((2,)), dma((2,)), dma((1,)), dma((1,)),
        ],
        compiler_params=pltpu.CompilerParams(collective_id=0, has_side_effects=True, vmem_limit_bytes=60 * 1024 * 1024),
        name="response",
    )(occ, idx, wave, resp, grad, local, *consts)


def shards(wave_coeff, response_coeff, band_index, occupation, local_kernel, gradient_kernel):
    return run(wave_coeff, response_coeff, occupation, band_index, gradient_kernel, local_kernel)


def solution(mesh):
    return jax.shard_map(
        shards,
        mesh=mesh,
        in_specs=(
            P(("pool", "slab"), None, None, None),
            P(("pool", "slab"), None, None, None),
            P(("pool", "slab")),
            P(),
            P("slab", None),
            P("slab", None),
        ),
        out_specs=P("slab", "pool"),
        check_vma=False,
    )
```

```python
import math

import numpy as np
import jax
import jax.numpy as jnp
from jax import lax
from jax.experimental import pallas as pl
from jax.experimental.pallas import tpu as pltpu
from jax.sharding import PartitionSpec as P

MESH = pl.DeviceIdType.MESH
full_turn = 2.0 * math.pi
N = 96
BL = 3072
NB = 9216 // BL
STEP = 97


def np_tables():
    k = np.arange(N)
    ang = (np.outer(k, k) % N) * (2 * np.pi / N)
    c, s = np.cos(ang) / np.sqrt(N), np.sin(ang) / np.sqrt(N)
    t = np.block([[c, -s], [s, c]])
    return t, np.cos(ang) + np.sin(ang)


def y_tables(t):
    outs = []
    for skip in (0, 32):
        w = np.zeros((256, 256))
        for s in range(2):
            for r in range(2):
                w[128 * s + skip:128 * s + skip + 96, 128 * r:128 * r + 96] = t[96 * r:96 * r + 96, 96 * s:96 * s + 96].T
        outs.append(w)
    return outs


def dense_tables(hu):
    outs = []
    for j in range(3):
        w = np.zeros((256, 128))
        for l in range(128):
            q, ky = divmod(128 * j + l, 96)
            w[(q - j) * 128:(q - j) * 128 + 96, l] = hu[ky]
        outs.append(w)
    return np.stack(outs)


def inverse_tables(hu):
    hye = np.zeros((128, 128))
    hye[:N] = hu[:, (np.arange(128) - 16) % N] / N
    return [hu / math.sqrt(N), hye]


def x_table(hu):
    w = np.zeros((16, 16, 32, 8))
    for p in range(16):
        for i in range(10):
            w[p, i, :, :3] = (hu[(6 * p - 2 + i) % N] / N).reshape(32, 3)
    w = w.reshape(256, 256)
    hi = w.astype(jnp.bfloat16).astype(np.float64)
    return np.concatenate([hi, hi, w - hi], axis=1)


def halves(v):
    hi = v.astype(jnp.bfloat16)
    return hi, (v - hi.astype(jnp.float32)).astype(jnp.bfloat16)


def close(a, b):
    (ah, al), (bh, bl) = halves(a), halves(b)
    return jnp.dot(jnp.concatenate([ah, ah, al], axis=1), jnp.concatenate([bh, bl, bh], axis=0), preferred_element_type=jnp.float32)


def kernel(occupation, numbers, wave, resp, grad, local, *refs):
    tables, out, held, refs = refs[:7], refs[7], refs[8:15], refs[15:]
    (occ, idx, cc, rs, bw, br, d, pbuf, s, f1, t2, f3, zbuf, rbuf, zp, zpr, zv, zvr, q, a, xo, b, gr, flat, gl, pot,
     csem, tsem, gsem, osem, p_snd, p_rcv, s1, r1, s3, r3, sp, rp, sv, rv, sa, ra, sb, rb, sg, rg) = refs
    t_ref, wy, yd, hx, hz, hye, hxe = held
    f32, bf = jnp.float32, jnp.bfloat16
    pool, slab = lax.axis_index("pool"), lax.axis_index("slab")
    y, x = pool // 4, pool % 4
    zc, core = slab // 2, slab % 2
    other = 1 - core

    def load(k, blk):
        return pltpu.make_async_copy((wave, resp)[k].at[0, :, :, pl.ds(blk * BL, BL)], cc.at[blk, k], csem.at[blk])

    early = [pltpu.make_async_copy(tables[n], held[n], tsem.at[n]) for n in range(2)]
    late = [pltpu.make_async_copy(tables[n], held[n], tsem.at[n]) for n in range(2, 7)]
    for cp in early:
        cp.start()
    for blk in range(NB):
        for k in range(2):
            load(k, blk).start()
    for cp in late:
        cp.start()
    weights = [pltpu.make_async_copy(occupation, occ, osem.at[0]), pltpu.make_async_copy(numbers, idx, osem.at[1])]
    for cp in weights:
        cp.start()
    for k, src in enumerate((grad, local)):
        for lo, to, size in ((0, 384, 9216), (9216 - 384, 0, 384), (0, 9600, 384)):
            pltpu.make_async_copy(src.at[:, pl.ds(lo, size)], flat.at[k, :, pl.ds(to, size)], gsem.at[0]).start()

    def drain(ref, sem):
        pltpu.make_async_copy(ref, ref, sem).wait()


    def dev(p, sl):
        return {"pool": p, "slab": sl}

    def plane(k):
        dc, dp = k // 16, k % 16
        c2 = (core + dc) % 2
        p2 = (pool + dp) % 16
        return c2, p2, dev(p2, zc * 2 + c2)

    barrier = pltpu.get_barrier_semaphore()

    def hail(who):
        pl.semaphore_signal(barrier, inc=1, device_id=who, device_id_type=MESH)

    for k in range(1, 32):
        hail(plane(k)[2])
    for dz in range(1, 8):
        hail(dev(pool, (slab + 2 * dz) % 16))
    hail(dev(pool, (slab + 15 + 2 * core) % 16))
    for r in range(12, 16):
        hail(dev(r, (slab + (1 if r < 14 else 15)) % 16))

    def send(src, dst, ssem, rsem, who):
        cp = pltpu.make_async_remote_copy(src_ref=src, dst_ref=dst, send_sem=ssem, recv_sem=rsem, device_id=who, device_id_type=MESH)
        cp.start()
        return cp

    for ref in (q, a, b):
        ref[...] = jnp.zeros_like(ref)
    for cp in early:
        cp.wait()

    def first_phase(blk, carry):
        drain(cc.at[blk], csem.at[blk])
        t = t_ref[...]
        for k, dst in enumerate((bw, br)):
            c = jnp.concatenate([cc[blk, k, 0], cc[blk, k, 1]], axis=0)
            zb = jnp.dot(t, c, preferred_element_type=f32).astype(bf)
            groups = BL // 384
            for row, (start, lo) in enumerate(((0, 0), (96, 0), (192, 0), (256, 256))):
                lhs = jnp.concatenate([
                    jnp.concatenate([zb[96 * r:96 * r + 96, 384 * n + start:384 * n + start + 128] for r in range(2)], axis=1)
                    for n in range(groups)], axis=0)
                res = jnp.dot(lhs, wy[lo:lo + 256], preferred_element_type=f32)
                for n in range(groups):
                    base = (blk * (BL // 96) + 4 * n + row) * STEP
                    for r in range(2):
                        dst[r, pl.ds(base, 96), :] = res[96 * n:96 * n + 96, 128 * r:128 * r + 128]
        return carry

    def to_space(chunk, planes):
        t = t_ref[...]
        weight = occ[idx[0]].astype(f32) * (1.0 / 256.0)
        for lo in (0, 4):
            spaces = []
            for src in (bw, br):
                parts = []
                for k, i in planes[lo:lo + 4]:
                    parts.append(jnp.concatenate([src[r, pl.ds(32 * chunk + 8 * k + i, 96, stride=STEP), :].astype(bf) for r in range(2)], axis=0))
                spaces.append(jnp.dot(t, jnp.concatenate(parts, axis=1), preferred_element_type=f32))
            v, w = spaces
            rho = ((v[:96] * w[:96] + v[96:] * w[96:]) * weight).astype(bf)
            for n, (k, i) in enumerate(planes[lo:lo + 4]):
                rs[k, pl.ds(i * 96, 96), :] = rho[:, 128 * n:128 * n + 128]

    def to_waves(u, j):
        lhs = jnp.concatenate([rs[j], rs[j + 1]], axis=1)
        col = jnp.dot(lhs, yd[j], preferred_element_type=f32)
        col = jnp.concatenate([col[96 * i:96 * i + 96] for i in range(8)], axis=1)
        gx = jnp.dot(hx[...], jnp.concatenate(halves(col), axis=0), preferred_element_type=f32)
        for i in range(8):
            d[u, pl.ds(i, 96, stride=9), :] = gx[:, 128 * i:128 * i + 128]

    def unit(u):
        c, j = divmod(u, 3)
        with jax.named_scope(f"unit{u}"):
            if j == 0:
                to_space(c, [(k, i) for i in range(4) for k in range(2)])
                to_space(c, [(k, i) for i in range(4, 8) for k in range(2)])
            else:
                to_space(c, [(j + 1, i) for i in range(8)])
            to_waves(u, j)


    def order(u, m, along):
        ax = (3 * u + m + along) % 2
        return (x, y)[ax], ax

    def at(ax, pos):
        return dev(y * 4 + pos, slab) if ax == 0 else dev(pos * 4 + x, slab)

    def units(c):
        return range(3 * c, 3 * c + 3)

    def start_pair(u):
        send(d.at[u, pl.ds(pl.multiple_of(other * 432, 432), 432)], pbuf.at[u], p_snd.at[0], p_rcv.at[u], dev(pool, zc * 2 + other))

    def start_a(u):
        with jax.named_scope(f"a{u}"):
            drain(pbuf.at[u], p_rcv.at[u])
            for n in range(48):
                s[u, n // 12, n // 3 % 4, n % 3] = d[u, pl.ds(core * 432 + 9 * n, 8), :] + pbuf[u, pl.ds(9 * n, 8), :]
            for m in range(3):
                pos, ax = order(u, m, 0)
                for k in (2, 1, 3):
                    to = (pos + k) % 4
                    src = s.at[u, :, to, m] if ax == 0 else s.at[u, to, :, m]
                    send(src, f1.at[u, m, k - 1], s1.at[0], r1.at[u], at(ax, to))

    def start_b(u):
        with jax.named_scope(f"b{u}"):
            drain(f1.at[u], r1.at[u])
            for m in range(3):
                pos, ax = order(u, m, 0)
                part = s[u, :, pos, m] if ax == 0 else s[u, pos, :, m]
                for k in (1, 3, 2):
                    part = part + f1[u, m, k - 1]
                t2[u, m] = part
                pos, ax = order(u, m, 1)
                for k in (2, 1, 3):
                    to = (pos + k) % 4
                    send(t2.at[u, m, to], f3.at[u, m, k - 1], s3.at[0], r3.at[u // 3], at(ax, to))

    lane = lax.broadcasted_iota(jnp.int32, (8, 128), 1)

    def finish(c):
        parts = {}
        drain(f3.at[pl.ds(3 * c, 3)], r3.at[c])
        for u in units(c):
            for m in range(3):
                part = t2[u, m, order(u, m, 1)[0]]
                for k in (1, 3, 2):
                    part = part + f3[u, m, k - 1]
                parts[u - 3 * c, m] = part
        for m in range(3):
            v = jnp.concatenate([parts[j, m] for j in range(3)], axis=1)
            for k in range(4):
                w = v if k == 0 else pltpu.roll(v, 384 - 96 * k, 1)
                zbuf[32 * c + 8 * k:32 * c + 8 * k + 8, 128 * m:128 * m + 128] = jnp.where(lane < 96, w[:, :128], 0.0)
        rows = jnp.concatenate([zbuf[32 * c:32 * c + 32, 128 * m:128 * m + 128] for m in range(3)], axis=0)
        both = close(rows, hye[...])
        for m in range(3):
            rbuf[m, 32 * c:32 * c + 32, :] = both[32 * m:32 * m + 32]
        for zd in ((0, 1), (2, 3, 4), (5, 6, 7))[c]:
            for m in range(3):
                zp[zd, 12 * m:12 * m + 12, :] = rbuf[m, 12 * zd:12 * zd + 12, :]
            slot = (zd - zc + 15) % 8
            cp = pltpu.make_async_remote_copy(src_ref=zp.at[zd], dst_ref=zpr.at[slot], send_sem=sp.at[0], recv_sem=rp.at[0], device_id=dev(pool, 2 * zd + core), device_id_type=MESH)
            pl.when(zc != zd)(cp.start)

    with jax.named_scope("first_phase"):
        lax.fori_loop(0, NB, first_phase, 0)
    for cp in late + weights:
        cp.wait()
    unit(0)
    with jax.named_scope("barrier"):
        pl.semaphore_wait(barrier, 39 + 16 * (pool // 12))
    start_pair(0)
    for u in range(1, 9):
        unit(u)
        start_pair(u)
        if u >= 2:
            start_a(u - 2)
        if u >= 7:
            start_b(u - 7)
    start_a(7)
    start_b(2)
    start_a(8)
    for u in (3, 4, 5):
        start_b(u)
    with jax.named_scope("finish0"):
        finish(0)
    for u in (6, 7, 8):
        start_b(u)
    with jax.named_scope("finish1"):
        finish(1)
    with jax.named_scope("finish2"):
        finish(2)

    with jax.named_scope("solve"):
        zk = zbuf[...]
        vh = close(hz[...], zk)
        kz = lax.broadcasted_iota(jnp.int32, (96, 128), 0)
        ky = lax.broadcasted_iota(jnp.int32, (96, 128), 1)
        qz = jnp.where(2 * kz >= N, kz - N, kz)
        qy = jnp.where(2 * ky >= N, ky - N, ky)
        zy = qz * qz + qy * qy
        scaled = []
        for m in range(3):
            kx = jnp.full((96, 128), 1, jnp.int32) * (3 * (core * 16 + pool) + m)
            qx = jnp.where(2 * kx >= N, kx - N, kx)
            squared = (zy + qx * qx).astype(f32) * ((full_turn / N) ** 2)
            screen = jnp.where(squared > 0, full_turn / jnp.where(squared > 0, squared, 1.0), 0.0)
            scaled.append(vh[:, 128 * m:128 * m + 128] * screen)
        vz = close(hz[...], jnp.concatenate(scaled, axis=1))
        both = close(jnp.concatenate([vz[:, 128 * m:128 * m + 128] for m in range(3)], axis=0), hye[...])
        for m in range(3):
            for zd in range(8):
                zv[zd, 12 * m:12 * m + 12, :] = both[96 * m + 12 * zd:96 * m + 12 * zd + 12]

    with jax.named_scope("zstage"):
        def col(k):
            return dev(pool, ((zc + k) % 8) * 2 + core)
        for k in (4, 3, 5, 2, 6, 1, 7):
            send(zv.at[(zc + k) % 8], zvr.at[k - 1], sv.at[0], rv.at[0], col(k))
        drain(flat, gsem.at[0])
        odd = pool % 2
        wide = lax.broadcasted_iota(jnp.int32, (6, 128), 1)
        for k in range(2):
            v = flat[k, :, pl.ds(pl.multiple_of(576 * pool - 64 * odd, 128), 1408)]
            v = jnp.where(odd == 1, pltpu.roll(v, 1408 - 64, 1), v)
            wins = [v[:, 176 + 96 * w:304 + 96 * w] for w in range(-1, 11)]
            for w in range(10):
                gl[k, pl.ds(w, 6, stride=16), :] = jnp.where(wide < 16, wins[w + 2], jnp.where(wide >= 112, wins[w], wins[w + 1]))
        send(gl.at[0, pl.ds(80, 16)], gr.at[0], sg.at[0], rg.at[0], dev(pool, (slab + 1) % 16))
        send(gl.at[0, pl.ds(0, 16)], gr.at[1], sg.at[0], rg.at[0], dev(pool, (slab + 15) % 16))

    me = core * 16 + pool
    mine = pl.ds(pl.multiple_of(me * 8, 8), 3)

    def deal(rows):
        for dc in range(2):
            c2 = (core + dc) % 2
            for r in rows:
                src = q.at[pl.ds(pl.multiple_of((c2 * 16 + r) * 8, 8), 3)]
                cp = pltpu.make_async_remote_copy(src_ref=src, dst_ref=a.at[mine], send_sem=sa.at[0], recv_sem=ra.at[0], device_id=dev(r, zc * 2 + c2), device_id_type=MESH)
                if dc:
                    cp.start()
                else:
                    pl.when(pool != r)(cp.start)

    with jax.named_scope("rows_rho"):
        drain(zpr, rp.at[0])
        f = zp[zc]
        for k in range(7):
            f = f + zpr[k]
        for c2 in range(2):
            for m in range(3):
                base = c2 * 128 + m
                rho6 = f[12 * m + 6 * c2:12 * m + 6 * c2 + 6]
                q[pl.ds(base, 6, stride=8), :] = rho6
                q[pl.ds(base + 96, 2, stride=8), :] = rho6[:2]
                q[pl.ds(base + 112, 2, stride=8), :] = rho6[4:]
        deal((0, 1, 2, 3, 4, 5, 12, 13, 14, 15))
    with jax.named_scope("rows_v"):
        drain(zvr, rv.at[0])
        f = zv[zc]
        for k in range(7):
            f = f + zvr[k]
        for c2 in range(2):
            for m in range(3):
                q[pl.ds(c2 * 128 + m + 48, 6, stride=8), :] = f[12 * m + 6 * c2:12 * m + 6 * c2 + 6]
        deal(range(6, 12))
    with jax.named_scope("rows_out"):
        a[mine, :] = q[pl.ds(pl.multiple_of((core * 16 + pool) * 8, 8), 3), :]
        drain(a.at[pl.ds(0, 93)], ra.at[0])
    with jax.named_scope("rows_back"):
        hi, lo = halves(a[...])
        xo[...] = jnp.dot(hxe[...], jnp.concatenate([hi, lo, hi], axis=0), preferred_element_type=f32).reshape(16, 16, 128)
        edge = pool // 12
        aim = (slab + 16 + edge * (2 * (pool // 14) - 1)) % 16
        for k in range(1, 16):
            p2 = (pool + k) % 16
            send(xo.at[p2, pl.ds(0, 10)], b.at[pool, pl.ds(0, 10)], sb.at[0], rb.at[0], dev(p2, aim))

        def across():
            return pltpu.make_async_remote_copy(src_ref=xo.at[pool, pl.ds(0, 10)], dst_ref=b.at[pool, pl.ds(0, 10)], send_sem=sb.at[1], recv_sem=rb.at[1], device_id=dev(pool, aim), device_id_type=MESH)

        @pl.when(edge == 0)
        def _():
            b[pool] = xo[pool]

        @pl.when(edge == 1)
        def _():
            across().start()
            across().wait()
        drain(gr, rg.at[0])
        drain(a.at[pl.ds(0, 150)], rb.at[0])

    with jax.named_scope("final"):
        def up(v, ax):
            return pltpu.roll(v, v.shape[ax] - 1, ax)

        def down(v, ax):
            return pltpu.roll(v, 1, ax)
        g = [gl[0, pl.ds(16 * n, 16), :] for n in range(6)]
        rhos = [b[n] for n in (14, 15, 0, 1, 2, 3, 4, 5, 12, 13)]
        flux = []
        for n in range(8):
            coef = gr[0] if n == 0 else gr[1] if n == 7 else g[n - 1]
            flux.append(coef * ((rhos[n + 2] - rhos[n]) * 0.5))
        for n in range(6):
            rho, coef = rhos[n + 2], g[n]
            div = (flux[n + 2] - flux[n]) * 0.5
            for ax in (0, 1):
                slope = coef * ((up(rho, ax) - down(rho, ax)) * 0.5)
                div = div + (up(slope, ax) - down(slope, ax)) * 0.5
            pot[pl.ds(16 * n, 16), :] = b[6 + n] + gl[1, pl.ds(16 * n, 16), :] * rho - div
        row640 = lax.broadcasted_iota(jnp.int32, (6, 640), 1)
        whole = jnp.zeros((6, 640), f32)
        for w in range(6):
            piece = jnp.concatenate([pot[pl.ds(w + 2, 6, stride=16), :], jnp.zeros((6, 512), f32)], axis=1)
            piece = pltpu.roll(piece, (96 * w - 16) % 640, 1)
            whole = jnp.where((row640 >= 96 * w) & (row640 < 96 * w + 96), piece, whole)
        out[...] = whole[:, :576]

    with jax.named_scope("sent"):
        for ref, sem in ((pbuf, p_snd), (f1, s1), (f3, s3), (zpr, sp), (zvr, sv), (gr, sg), (a.at[pl.ds(0, 93)], sa), (a.at[pl.ds(0, 150)], sb)):
            drain(ref, sem.at[0])


def run(wave, resp, occ, idx, grad, local):
    t, hu = np_tables()
    f32, bf = jnp.float32, jnp.bfloat16
    consts = [jnp.asarray(v, bf) for v in (t, np.concatenate(y_tables(t)), dense_tables(hu), np.concatenate([hu, hu], axis=1))]
    consts += [jnp.asarray(v, f32) for v in inverse_tables(hu)]
    consts.append(jnp.asarray(x_table(hu), bf))
    vm, hbm = pl.BlockSpec(memory_space=pltpu.VMEM), pl.BlockSpec(memory_space=pltpu.HBM)
    dma = pltpu.SemaphoreType.DMA
    buf = lambda *dims: pltpu.VMEM(dims, f32)
    return pl.pallas_call(
        kernel,
        out_shape=pltpu.VMEM((6, 576), f32),
        in_specs=[hbm] * (6 + len(consts)),
        out_specs=vm,
        scratch_shapes=[
            *(pltpu.VMEM(v.shape, v.dtype) for v in consts),
            pltpu.SMEM((256,), jnp.int32), pltpu.SMEM((1,), jnp.int32),
            pltpu.VMEM((NB, 2, 2, 96, BL), bf), pltpu.VMEM((4, 768, 128), bf),
            buf(2, 96 * STEP, 128), buf(2, 96 * STEP, 128), buf(9, 864, 128), buf(9, 432, 128), buf(9, 4, 4, 3, 8, 128),
            buf(9, 3, 3, 4, 8, 128), buf(9, 3, 4, 8, 128), buf(9, 3, 3, 8, 128), buf(96, 384), buf(3, 96, 128),
            buf(8, 36, 128), buf(7, 36, 128), buf(8, 36, 128), buf(7, 36, 128), buf(256, 128), buf(256, 128),
            buf(16, 16, 128), buf(16, 16, 128), buf(2, 16, 128), buf(2, 6, 9984), buf(2, 96, 128), buf(96, 128),
            dma((NB,)), dma((7,)), dma((1,)), dma((2,)), dma((1,)), dma((9,)), dma((1,)), dma((9,)), dma((1,)), dma((3,)),
            *(dma((1,)) for _ in range(6)), dma((2,)), dma((2,)), dma((1,)), dma((1,)),
        ],
        compiler_params=pltpu.CompilerParams(collective_id=0, has_side_effects=True, vmem_limit_bytes=60 * 1024 * 1024),
        name="response",
    )(occ, idx, wave, resp, grad, local, *consts)


def shards(wave_coeff, response_coeff, band_index, occupation, local_kernel, gradient_kernel):
    return run(wave_coeff, response_coeff, occupation, band_index, gradient_kernel, local_kernel)


def solution(mesh):
    return jax.shard_map(
        shards,
        mesh=mesh,
        in_specs=(
            P(("pool", "slab"), None, None, None),
            P(("pool", "slab"), None, None, None),
            P(("pool", "slab")),
            P(),
            P("slab", None),
            P("slab", None),
        ),
        out_specs=P("slab", "pool"),
        check_vma=False,
    )
```

```python
import math

import numpy as np
import jax
import jax.numpy as jnp
from jax import lax
from jax.experimental import pallas as pl
from jax.experimental.pallas import tpu as pltpu
from jax.sharding import PartitionSpec as P

MESH = pl.DeviceIdType.MESH
full_turn = 2.0 * math.pi
N = 96
BL = 3072
NB = 9216 // BL
STEP = 97


def np_tables():
    k = np.arange(N)
    ang = (np.outer(k, k) % N) * (2 * np.pi / N)
    c, s = np.cos(ang) / np.sqrt(N), np.sin(ang) / np.sqrt(N)
    t = np.block([[c, -s], [s, c]])
    return t, np.cos(ang) + np.sin(ang)


def y_tables(t):
    outs = []
    for skip in (0, 32):
        w = np.zeros((256, 256))
        for s in range(2):
            for r in range(2):
                w[128 * s + skip:128 * s + skip + 96, 128 * r:128 * r + 96] = t[96 * r:96 * r + 96, 96 * s:96 * s + 96].T
        outs.append(w)
    return outs


def dense_tables(hu):
    outs = []
    for j in range(3):
        w = np.zeros((256, 128))
        for l in range(128):
            q, ky = divmod(128 * j + l, 96)
            w[(q - j) * 128:(q - j) * 128 + 96, l] = hu[ky]
        outs.append(w)
    return np.stack(outs)


def inverse_tables(hu):
    hye = np.zeros((128, 128))
    hye[:N] = hu[:, (np.arange(128) - 16) % N] / N
    return [hu / math.sqrt(N), hye]


def x_table(hu):
    w = np.zeros((16, 16, 32, 8))
    for p in range(16):
        for i in range(10):
            w[p, i, :, :3] = (hu[(6 * p - 2 + i) % N] / N).reshape(32, 3)
    w = w.reshape(256, 256)
    hi = w.astype(jnp.bfloat16).astype(np.float64)
    return np.concatenate([hi, hi, w - hi], axis=1)


def halves(v):
    hi = v.astype(jnp.bfloat16)
    return hi, (v - hi.astype(jnp.float32)).astype(jnp.bfloat16)


def close(a, b):
    (ah, al), (bh, bl) = halves(a), halves(b)
    return jnp.dot(jnp.concatenate([ah, ah, al], axis=1), jnp.concatenate([bh, bl, bh], axis=0), preferred_element_type=jnp.float32)


def kernel(occupation, numbers, wave, resp, grad, local, *refs):
    tables, out, held, refs = refs[:7], refs[7], refs[8:15], refs[15:]
    (occ, idx, cc, rs, bw, br, d, pbuf, s, f1, t2, f3, zbuf, rbuf, zp, zpr, zv, zvr, q, a, xo, b, gr, flat, gl, pot,
     csem, tsem, gsem, osem, p_snd, p_rcv, s1, r1, s3, r3, sp, rp, sv, rv, sa, ra, sb, rb, sg, rg) = refs
    t_ref, wy, yd, hx, hz, hye, hxe = held
    f32, bf = jnp.float32, jnp.bfloat16
    pool, slab = lax.axis_index("pool"), lax.axis_index("slab")
    y, x = pool // 4, pool % 4
    zc, core = slab // 2, slab % 2
    other = 1 - core

    def load(k, blk):
        return pltpu.make_async_copy((wave, resp)[k].at[0, :, :, pl.ds(blk * BL, BL)], cc.at[blk, k], csem.at[blk])

    early = [pltpu.make_async_copy(tables[n], held[n], tsem.at[n]) for n in range(2)]
    late = [pltpu.make_async_copy(tables[n], held[n], tsem.at[n]) for n in range(2, 7)]
    for cp in early:
        cp.start()
    for blk in range(NB):
        for k in range(2):
            load(k, blk).start()
    for cp in late:
        cp.start()
    weights = [pltpu.make_async_copy(occupation, occ, osem.at[0]), pltpu.make_async_copy(numbers, idx, osem.at[1])]
    for cp in weights:
        cp.start()
    for k, src in enumerate((grad, local)):
        for lo, to, size in ((0, 384, 9216), (9216 - 384, 0, 384), (0, 9600, 384)):
            pltpu.make_async_copy(src.at[:, pl.ds(lo, size)], flat.at[k, :, pl.ds(to, size)], gsem.at[0]).start()

    def drain(ref, sem):
        pltpu.make_async_copy(ref, ref, sem).wait()


    def dev(p, sl):
        return {"pool": p, "slab": sl}

    def plane(k):
        dc, dp = k // 16, k % 16
        c2 = (core + dc) % 2
        p2 = (pool + dp) % 16
        return c2, p2, dev(p2, zc * 2 + c2)

    barrier = pltpu.get_barrier_semaphore()

    def hail(who):
        pl.semaphore_signal(barrier, inc=1, device_id=who, device_id_type=MESH)

    for k in range(1, 32):
        hail(plane(k)[2])
    for dz in range(1, 8):
        hail(dev(pool, (slab + 2 * dz) % 16))
    hail(dev(pool, (slab + 15 + 2 * core) % 16))
    for r in range(12, 16):
        hail(dev(r, (slab + (1 if r < 14 else 15)) % 16))

    def send(src, dst, ssem, rsem, who):
        cp = pltpu.make_async_remote_copy(src_ref=src, dst_ref=dst, send_sem=ssem, recv_sem=rsem, device_id=who, device_id_type=MESH)
        cp.start()
        return cp

    for ref in (q, a, b):
        ref[...] = jnp.zeros_like(ref)
    for cp in early:
        cp.wait()

    def first_phase(blk, carry):
        drain(cc.at[blk], csem.at[blk])
        t = t_ref[...]
        for k, dst in enumerate((bw, br)):
            c = jnp.concatenate([cc[blk, k, 0], cc[blk, k, 1]], axis=0)
            zb = jnp.dot(t, c, preferred_element_type=f32).astype(bf)
            groups = BL // 384
            for row, (start, lo) in enumerate(((0, 0), (96, 0), (192, 0), (256, 256))):
                lhs = jnp.concatenate([
                    jnp.concatenate([zb[96 * r:96 * r + 96, 384 * n + start:384 * n + start + 128] for r in range(2)], axis=1)
                    for n in range(groups)], axis=0)
                res = jnp.dot(lhs, wy[lo:lo + 256], preferred_element_type=f32)
                for n in range(groups):
                    base = (blk * (BL // 96) + 4 * n + row) * STEP
                    for r in range(2):
                        dst[r, pl.ds(base, 96), :] = res[96 * n:96 * n + 96, 128 * r:128 * r + 128]
        return carry

    def to_space(chunk, planes):
        t = t_ref[...]
        weight = occ[idx[0]].astype(f32) * (1.0 / 256.0)
        for lo in (0, 4):
            spaces = []
            for src in (bw, br):
                parts = []
                for k, i in planes[lo:lo + 4]:
                    parts.append(jnp.concatenate([src[r, pl.ds(32 * chunk + 8 * k + i, 96, stride=STEP), :].astype(bf) for r in range(2)], axis=0))
                spaces.append(jnp.dot(t, jnp.concatenate(parts, axis=1), preferred_element_type=f32))
            v, w = spaces
            rho = ((v[:96] * w[:96] + v[96:] * w[96:]) * weight).astype(bf)
            for n, (k, i) in enumerate(planes[lo:lo + 4]):
                rs[k, pl.ds(i * 96, 96), :] = rho[:, 128 * n:128 * n + 128]

    def to_waves(u, j):
        lhs = jnp.concatenate([rs[j], rs[j + 1]], axis=1)
        col = jnp.dot(lhs, yd[j], preferred_element_type=f32)
        col = jnp.concatenate([col[96 * i:96 * i + 96] for i in range(8)], axis=1)
        gx = jnp.dot(hx[...], jnp.concatenate(halves(col), axis=0), preferred_element_type=f32)
        for i in range(8):
            d[u, pl.ds(i, 96, stride=9), :] = gx[:, 128 * i:128 * i + 128]

    def unit(u):
        c, j = divmod(u, 3)
        with jax.named_scope(f"unit{u}"):
            if j == 0:
                to_space(c, [(k, i) for i in range(4) for k in range(2)])
                to_space(c, [(k, i) for i in range(4, 8) for k in range(2)])
            else:
                to_space(c, [(j + 1, i) for i in range(8)])
            to_waves(u, j)


    def order(u, m, along):
        ax = (3 * u + m + along) % 2
        return (x, y)[ax], ax

    def at(ax, pos):
        return dev(y * 4 + pos, slab) if ax == 0 else dev(pos * 4 + x, slab)

    def units(c):
        return range(3 * c, 3 * c + 3)

    def start_pair(u):
        send(d.at[u, pl.ds(pl.multiple_of(other * 432, 432), 432)], pbuf.at[u], p_snd.at[0], p_rcv.at[u], dev(pool, zc * 2 + other))

    def start_a(u):
        with jax.named_scope(f"a{u}"):
            drain(pbuf.at[u], p_rcv.at[u])
            for n in range(48):
                s[u, n // 12, n // 3 % 4, n % 3] = d[u, pl.ds(core * 432 + 9 * n, 8), :] + pbuf[u, pl.ds(9 * n, 8), :]
            for m in range(3):
                pos, ax = order(u, m, 0)
                for k in (2, 1, 3):
                    to = (pos + k) % 4
                    src = s.at[u, :, to, m] if ax == 0 else s.at[u, to, :, m]
                    send(src, f1.at[u, m, k - 1], s1.at[0], r1.at[u], at(ax, to))

    def start_b(u):
        with jax.named_scope(f"b{u}"):
            drain(f1.at[u], r1.at[u])
            for m in range(3):
                pos, ax = order(u, m, 0)
                part = s[u, :, pos, m] if ax == 0 else s[u, pos, :, m]
                for k in (1, 3, 2):
                    part = part + f1[u, m, k - 1]
                t2[u, m] = part
                pos, ax = order(u, m, 1)
                for k in (2, 1, 3):
                    to = (pos + k) % 4
                    send(t2.at[u, m, to], f3.at[u, m, k - 1], s3.at[0], r3.at[u // 3], at(ax, to))

    lane = lax.broadcasted_iota(jnp.int32, (8, 128), 1)

    def finish(c):
        parts = {}
        drain(f3.at[pl.ds(3 * c, 3)], r3.at[c])
        for u in units(c):
            for m in range(3):
                part = t2[u, m, order(u, m, 1)[0]]
                for k in (1, 3, 2):
                    part = part + f3[u, m, k - 1]
                parts[u - 3 * c, m] = part
        for m in range(3):
            v = jnp.concatenate([parts[j, m] for j in range(3)], axis=1)
            for k in range(4):
                w = v if k == 0 else pltpu.roll(v, 384 - 96 * k, 1)
                zbuf[32 * c + 8 * k:32 * c + 8 * k + 8, 128 * m:128 * m + 128] = jnp.where(lane < 96, w[:, :128], 0.0)
        rows = jnp.concatenate([zbuf[32 * c:32 * c + 32, 128 * m:128 * m + 128] for m in range(3)], axis=0)
        both = close(rows, hye[...])
        for m in range(3):
            rbuf[m, 32 * c:32 * c + 32, :] = both[32 * m:32 * m + 32]
        for zd in ((0, 1), (2, 3, 4), (5, 6, 7))[c]:
            for m in range(3):
                zp[zd, 12 * m:12 * m + 12, :] = rbuf[m, 12 * zd:12 * zd + 12, :]
            slot = (zd - zc + 15) % 8
            cp = pltpu.make_async_remote_copy(src_ref=zp.at[zd], dst_ref=zpr.at[slot], send_sem=sp.at[0], recv_sem=rp.at[0], device_id=dev(pool, 2 * zd + core), device_id_type=MESH)
            pl.when(zc != zd)(cp.start)

    with jax.named_scope("first_phase"):
        lax.fori_loop(0, NB, first_phase, 0)
    for cp in late + weights:
        cp.wait()
    unit(0)
    with jax.named_scope("barrier"):
        pl.semaphore_wait(barrier, 39 + 16 * (pool // 12))
    start_pair(0)
    for u in range(1, 9):
        unit(u)
        start_pair(u)
        if u >= 2:
            start_a(u - 2)
        if u >= 7:
            start_b(u - 7)
    start_a(7)
    start_b(2)
    start_a(8)
    for u in range(3, 9):
        start_b(u)
    with jax.named_scope("finish0"):
        finish(0)
    with jax.named_scope("finish1"):
        finish(1)
    with jax.named_scope("finish2"):
        finish(2)

    with jax.named_scope("solve"):
        zk = zbuf[...]
        vh = close(hz[...], zk)
        kz = lax.broadcasted_iota(jnp.int32, (96, 128), 0)
        ky = lax.broadcasted_iota(jnp.int32, (96, 128), 1)
        qz = jnp.where(2 * kz >= N, kz - N, kz)
        qy = jnp.where(2 * ky >= N, ky - N, ky)
        zy = qz * qz + qy * qy
        scaled = []
        for m in range(3):
            kx = jnp.full((96, 128), 1, jnp.int32) * (3 * (core * 16 + pool) + m)
            qx = jnp.where(2 * kx >= N, kx - N, kx)
            squared = (zy + qx * qx).astype(f32) * ((full_turn / N) ** 2)
            screen = jnp.where(squared > 0, full_turn / jnp.where(squared > 0, squared, 1.0), 0.0)
            scaled.append(vh[:, 128 * m:128 * m + 128] * screen)
        vz = close(hz[...], jnp.concatenate(scaled, axis=1))
        both = close(jnp.concatenate([vz[:, 128 * m:128 * m + 128] for m in range(3)], axis=0), hye[...])
        for m in range(3):
            for zd in range(8):
                zv[zd, 12 * m:12 * m + 12, :] = both[96 * m + 12 * zd:96 * m + 12 * zd + 12]

    with jax.named_scope("zstage"):
        def col(k):
            return dev(pool, ((zc + k) % 8) * 2 + core)
        for k in (4, 3, 5, 2, 6, 1, 7):
            send(zv.at[(zc + k) % 8], zvr.at[k - 1], sv.at[0], rv.at[0], col(k))
        drain(flat, gsem.at[0])
        odd = pool % 2
        wide = lax.broadcasted_iota(jnp.int32, (6, 128), 1)
        for k in range(2):
            v = flat[k, :, pl.ds(pl.multiple_of(576 * pool - 64 * odd, 128), 1408)]
            v = jnp.where(odd == 1, pltpu.roll(v, 1408 - 64, 1), v)
            wins = [v[:, 176 + 96 * w:304 + 96 * w] for w in range(-1, 11)]
            for w in range(10):
                gl[k, pl.ds(w, 6, stride=16), :] = jnp.where(wide < 16, wins[w + 2], jnp.where(wide >= 112, wins[w], wins[w + 1]))
        send(gl.at[0, pl.ds(80, 16)], gr.at[0], sg.at[0], rg.at[0], dev(pool, (slab + 1) % 16))
        send(gl.at[0, pl.ds(0, 16)], gr.at[1], sg.at[0], rg.at[0], dev(pool, (slab + 15) % 16))

    me = core * 16 + pool
    mine = pl.ds(pl.multiple_of(me * 8, 8), 3)

    def deal(rows):
        for dc in range(2):
            c2 = (core + dc) % 2
            for r in rows:
                src = q.at[pl.ds(pl.multiple_of((c2 * 16 + r) * 8, 8), 3)]
                cp = pltpu.make_async_remote_copy(src_ref=src, dst_ref=a.at[mine], send_sem=sa.at[0], recv_sem=ra.at[0], device_id=dev(r, zc * 2 + c2), device_id_type=MESH)
                if dc:
                    cp.start()
                else:
                    pl.when(pool != r)(cp.start)

    with jax.named_scope("rows_rho"):
        drain(zpr, rp.at[0])
        f = zp[zc]
        for k in range(7):
            f = f + zpr[k]
        for c2 in range(2):
            for m in range(3):
                base = c2 * 128 + m
                rho6 = f[12 * m + 6 * c2:12 * m + 6 * c2 + 6]
                q[pl.ds(base, 6, stride=8), :] = rho6
                q[pl.ds(base + 96, 2, stride=8), :] = rho6[:2]
                q[pl.ds(base + 112, 2, stride=8), :] = rho6[4:]
        deal((0, 1, 2, 3, 4, 5, 12, 13, 14, 15))
    with jax.named_scope("rows_v"):
        drain(zvr, rv.at[0])
        f = zv[zc]
        for k in range(7):
            f = f + zvr[k]
        for c2 in range(2):
            for m in range(3):
                q[pl.ds(c2 * 128 + m + 48, 6, stride=8), :] = f[12 * m + 6 * c2:12 * m + 6 * c2 + 6]
        deal(range(6, 12))
    with jax.named_scope("rows_out"):
        a[mine, :] = q[pl.ds(pl.multiple_of((core * 16 + pool) * 8, 8), 3), :]
        drain(a.at[pl.ds(0, 93)], ra.at[0])
    with jax.named_scope("rows_back"):
        hi, lo = halves(a[...])
        xo[...] = jnp.dot(hxe[...], jnp.concatenate([hi, lo, hi], axis=0), preferred_element_type=f32).reshape(16, 16, 128)
        edge = pool // 12
        aim = (slab + 16 + edge * (2 * (pool // 14) - 1)) % 16
        for k in range(1, 16):
            p2 = (pool + k) % 16
            send(xo.at[p2, pl.ds(0, 10)], b.at[pool, pl.ds(0, 10)], sb.at[0], rb.at[0], dev(p2, aim))

        def across():
            return pltpu.make_async_remote_copy(src_ref=xo.at[pool, pl.ds(0, 10)], dst_ref=b.at[pool, pl.ds(0, 10)], send_sem=sb.at[1], recv_sem=rb.at[1], device_id=dev(pool, aim), device_id_type=MESH)

        @pl.when(edge == 0)
        def _():
            b[pool] = xo[pool]

        @pl.when(edge == 1)
        def _():
            across().start()
            across().wait()
        drain(gr, rg.at[0])
        drain(a.at[pl.ds(0, 150)], rb.at[0])

    with jax.named_scope("final"):
        def up(v, ax):
            return pltpu.roll(v, v.shape[ax] - 1, ax)

        def down(v, ax):
            return pltpu.roll(v, 1, ax)
        g = [gl[0, pl.ds(16 * n, 16), :] for n in range(6)]
        rhos = [b[n] for n in (14, 15, 0, 1, 2, 3, 4, 5, 12, 13)]
        flux = []
        for n in range(8):
            coef = gr[0] if n == 0 else gr[1] if n == 7 else g[n - 1]
            flux.append(coef * ((rhos[n + 2] - rhos[n]) * 0.5))
        for n in range(6):
            rho, coef = rhos[n + 2], g[n]
            div = (flux[n + 2] - flux[n]) * 0.5
            for ax in (0, 1):
                slope = coef * ((up(rho, ax) - down(rho, ax)) * 0.5)
                div = div + (up(slope, ax) - down(slope, ax)) * 0.5
            pot[pl.ds(16 * n, 16), :] = b[6 + n] + gl[1, pl.ds(16 * n, 16), :] * rho - div
        row640 = lax.broadcasted_iota(jnp.int32, (6, 640), 1)
        whole = jnp.zeros((6, 640), f32)
        for w in range(6):
            piece = jnp.concatenate([pot[pl.ds(w + 2, 6, stride=16), :], jnp.zeros((6, 512), f32)], axis=1)
            piece = pltpu.roll(piece, (96 * w - 16) % 640, 1)
            whole = jnp.where((row640 >= 96 * w) & (row640 < 96 * w + 96), piece, whole)
        out[...] = whole[:, :576]

    with jax.named_scope("sent"):
        for ref, sem in ((pbuf, p_snd), (f1, s1), (f3, s3), (zpr, sp), (zvr, sv), (gr, sg), (a.at[pl.ds(0, 93)], sa), (a.at[pl.ds(0, 150)], sb)):
            drain(ref, sem.at[0])


def run(wave, resp, occ, idx, grad, local):
    t, hu = np_tables()
    f32, bf = jnp.float32, jnp.bfloat16
    consts = [jnp.asarray(v, bf) for v in (t, np.concatenate(y_tables(t)), dense_tables(hu), np.concatenate([hu, hu], axis=1))]
    consts += [jnp.asarray(v, f32) for v in inverse_tables(hu)]
    consts.append(jnp.asarray(x_table(hu), bf))
    vm, hbm = pl.BlockSpec(memory_space=pltpu.VMEM), pl.BlockSpec(memory_space=pltpu.HBM)
    dma = pltpu.SemaphoreType.DMA
    buf = lambda *dims: pltpu.VMEM(dims, f32)
    return pl.pallas_call(
        kernel,
        out_shape=pltpu.VMEM((6, 576), f32),
        in_specs=[hbm] * (6 + len(consts)),
        out_specs=vm,
        scratch_shapes=[
            *(pltpu.VMEM(v.shape, v.dtype) for v in consts),
            pltpu.SMEM((256,), jnp.int32), pltpu.SMEM((1,), jnp.int32),
            pltpu.VMEM((NB, 2, 2, 96, BL), bf), pltpu.VMEM((4, 768, 128), bf),
            buf(2, 96 * STEP, 128), buf(2, 96 * STEP, 128), buf(9, 864, 128), buf(9, 432, 128), buf(9, 4, 4, 3, 8, 128),
            buf(9, 3, 3, 4, 8, 128), buf(9, 3, 4, 8, 128), buf(9, 3, 3, 8, 128), buf(96, 384), buf(3, 96, 128),
            buf(8, 36, 128), buf(7, 36, 128), buf(8, 36, 128), buf(7, 36, 128), buf(256, 128), buf(256, 128),
            buf(16, 16, 128), buf(16, 16, 128), buf(2, 16, 128), buf(2, 6, 9984), buf(2, 96, 128), buf(96, 128),
            dma((NB,)), dma((7,)), dma((1,)), dma((2,)), dma((1,)), dma((9,)), dma((1,)), dma((9,)), dma((1,)), dma((3,)),
            *(dma((1,)) for _ in range(6)), dma((2,)), dma((2,)), dma((1,)), dma((1,)),
        ],
        compiler_params=pltpu.CompilerParams(collective_id=0, has_side_effects=True, vmem_limit_bytes=60 * 1024 * 1024),
        name="response",
    )(occ, idx, wave, resp, grad, local, *consts)


def shards(wave_coeff, response_coeff, band_index, occupation, local_kernel, gradient_kernel):
    return run(wave_coeff, response_coeff, occupation, band_index, gradient_kernel, local_kernel)


def solution(mesh):
    return jax.shard_map(
        shards,
        mesh=mesh,
        in_specs=(
            P(("pool", "slab"), None, None, None),
            P(("pool", "slab"), None, None, None),
            P(("pool", "slab")),
            P(),
            P("slab", None),
            P("slab", None),
        ),
        out_specs=P("slab", "pool"),
        check_vma=False,
    )
```
